256 devices in a mesh: stripe: 2 (over z), row: 64 (over x, y), col: 2 (over core).
Axes of the slice: x: 8, y: 8, z: 2, core: 2. Of those that a mesh axis runs over, the one named last changes fastest.
The devices are a block of a 8x8x16 slice.
Arguments:
- coverage: int32 [32768, 4096], P(('stripe', 'row'), 'col'), parts along dimension 0, may hold values from 0 to 255
- fog_rows: float32 [64, 64], replicated, may hold values from 0.02 to 50
- fog_cols: float32 [16, 16], replicated, may hold values from 0.02 to 50
Outputs:
- dose: float32 [32768, 4096], P(('stripe', 'row'), 'col'), parts along dimension 0
The draws below stay inside these ranges and needn't reach their ends.
There are 2 independent parts, one for each index of `stripe`. The reference program is written for one: setup_inputs(seed, part) draws one part's arguments, and reference() takes and returns one part's arrays. A program takes and returns all parts, laid end to end along the dimension named above; an argument that names none is the same for every part. Nothing has to cross between parts.
All inputs are finite; a program needn't handle non-finite values.
Results may differ from the reference program's by a relative error of at most 0.0001.
Values sent between devices are 32-bit elements; how exact they have to be, the bound alone decides.
A program may use at most 64 MiB of HBM per device.

```python
import math
import jax
import jax.numpy as jnp
from jax import lax

BS = 32
FB = 256
HALO = 4
BSIG = 16
REACH = 40
PASSES = 2
NR = 16384
NC = 4096
FR = 64
FC = 16


def draw_coverage(key, part):
    first = jax.random.fold_in(key, 11)
    second = jax.random.fold_in(key, 12)
    third = jax.random.fold_in(key, 13)
    pixels = jax.random.randint(first, (NR, NC), 0, 256)
    levels = jax.random.randint(second, (NR // BS, NC // BS), 0, 5)
    regions = jax.random.randint(third, (NR // FB, NC // FB), 1, 4)
    levels_full = jnp.repeat(jnp.repeat(levels, BS, axis=0), BS, axis=1)
    regions_full = jnp.repeat(jnp.repeat(regions, FB, axis=0), FB, axis=1)
    return (pixels * levels_full * regions_full // 12).astype(jnp.int32)


def setup_inputs(seed: int = 0, part: int = 0) -> dict:
    streams_of = jax.random.split(jax.random.key(seed), 4)
    own_keys = jax.random.split(jax.random.fold_in(streams_of[3], part), 4)
    return {
        "coverage": draw_coverage(jax.random.fold_in(jax.random.fold_in(streams_of[3], part), 71), part),
        "fog_rows": jnp.clip(jnp.exp(jax.random.uniform(streams_of[1], (FR, FR), jnp.float32, math.log(0.02), math.log(50.0))), 0.02, 50.0),
        "fog_cols": jnp.clip(jnp.exp(jax.random.uniform(streams_of[2], (FC, FC), jnp.float32, math.log(0.02), math.log(50.0))), 0.02, 50.0),
    }


def fine_taps():
    offsets = jnp.arange(-HALO, HALO + 1).astype(jnp.float32)
    raw = jnp.exp(-0.5 * (offsets / 1.25) ** 2)
    return raw / jnp.sum(raw)

def blur_padded(padded, rows, cols):
    taps = fine_taps()
    across = taps[0] * padded[0:rows, :]
    for index in range(1, 2 * HALO + 1):
        across = across + taps[index] * padded[index:index + rows, :]
    result = taps[0] * across[:, 0:cols]
    for index in range(1, 2 * HALO + 1):
        result = result + taps[index] * across[:, index:index + cols]
    return result

def block_mean(field, size):
    rows, cols = field.shape
    return field.reshape(rows // size, size, cols // size, size).sum(axis=(1, 3)) / (size * size)

def spread_add(field, small, size, weight):
    rows, cols = field.shape
    return (field.reshape(rows // size, size, cols // size, size) + weight * small[:, None, :, None]).reshape(rows, cols)

def gauss_matrix(first, second):
    offsets = (first[:, None] - second[None, :]).astype(jnp.float32)
    values = jnp.exp(-0.5 * (offsets / BSIG) ** 2) / (BSIG * math.sqrt(2.0 * math.pi))
    return jnp.where(jnp.abs(offsets) <= REACH, values, jnp.zeros_like(values))

def reference(coverage, fog_rows, fog_cols):
    cover = coverage.astype(jnp.float32) / 255.0
    dose = jnp.ones((NR, NC), jnp.float32)
    row_norm = fog_rows / lax.optimization_barrier(jnp.sum(fog_rows, axis=1, keepdims=True))
    col_norm = fog_cols / lax.optimization_barrier(jnp.sum(fog_cols, axis=1, keepdims=True))
    coarse_cols = jnp.arange(NC // BS, dtype=jnp.int32)
    coarse_rows = jnp.arange(NR // BS, dtype=jnp.int32)
    across_gauss = gauss_matrix(coarse_cols, coarse_cols)
    down_gauss = gauss_matrix(coarse_rows, coarse_rows)
    high = lax.Precision.HIGHEST
    for step in range(PASSES):
        charge = dose * cover
        fine = blur_padded(jnp.pad(charge, HALO), NR, NC)
        back = block_mean(charge, BS)
        back_h = jnp.dot(back, across_gauss, precision=high)
        back_v = jnp.dot(down_gauss, back_h, precision=high)
        fogmean = block_mean(charge, FB)
        fog = jnp.dot(jnp.dot(row_norm, fogmean, precision=high), col_norm.T, precision=high)
        energy = spread_add(fine, back_v, BS, 0.6)
        energy = spread_add(energy, fog, FB, 0.4) / 2.0
        dose = dose + (0.5 - energy)
    return dose
```

```python
import math

import jax
import jax.numpy as jnp
from jax import lax
from jax.experimental import pallas as pl
from jax.experimental.pallas import tpu as pltpu
from jax.sharding import PartitionSpec as P

BS = 32
FB = 256
HALO = 4
BSIG = 16
REACH = 40
SIDE = 8
MESH = pl.DeviceIdType.MESH
F32 = jnp.float32
BF16 = jnp.bfloat16
I32 = jnp.int32
ORDER = (4, 3, 5, 2, 6, 1, 7)

TAPS = [math.exp(-(k * k) / (2 * 1.25**2)) for k in range(-HALO, HALO + 1)]
TAP_SCALE = 1.0 / sum(TAPS)
GAUSS_SCALE = 1.0 / (BSIG * math.sqrt(2.0 * math.pi))


def iota(shape, dim):
    return lax.broadcasted_iota(I32, shape, dim)


def onehot(condition):
    return jnp.where(condition, 1.0, 0.0).astype(F32)


def taps_of(offset):
    square = (offset * offset).astype(F32)
    value = jnp.exp(square * (-1.0 / (2 * 1.25**2))) * TAP_SCALE
    return jnp.where(jnp.abs(offset) <= HALO, value, 0.0)


def gauss_of(offset):
    square = (offset * offset).astype(F32)
    value = jnp.exp(square * (-0.5 / (BSIG * BSIG))) * GAUSS_SCALE
    return jnp.where(jnp.abs(offset) <= REACH, value, 0.0)


def split(value):
    high = value.astype(BF16)
    return high, (value - high.astype(F32)).astype(BF16)


def dot(a, b):
    return jnp.dot(a, b, preferred_element_type=F32)


def dot_exact(a, b):
    high, low = split(a)
    b = b.astype(BF16)
    return dot(high, b) + dot(low, b)


def exact_dot(a, b):
    high, low = split(b)
    a = a.astype(BF16)
    return dot(a, high) + dot(a, low)


def dot3(a, b):
    ah, al = split(a)
    bh, bl = split(b)
    return dot(ah, bh) + (dot(al, bh) + dot(ah, bl))


def correct_kernel(
    cov, fogr, fogc, x_out, coarse_out,
    ext, cb, rs, cs, hhi, hlo, tt, asum, qhi, qlo, h2hi, h2lo,
    s1, s2, sps, wcat, b0, b16, row24, mbuf, mext, pbuf, abuf, bext, ebuf, fr, fc,
    load_sem, fog_sem, halo_send, halo_recv,
    m_send, m_recv, a_send, a_recv, p_send, p_recv, e_send, e_recv,
    ms_send, ms_recv, bs_send, bs_recv,
):
    stripe = lax.axis_index("stripe")
    row = lax.axis_index("row")
    col = lax.axis_index("col")
    px = row // SIDE
    py = lax.rem(row, SIDE)
    other = 1 - col
    rows, cols = 256, cov.shape[1]
    cells = cols // BS
    wide = cols + 128
    last = SIDE * SIDE - 1

    loads = []
    for i in range(8):
        copy = pltpu.make_async_copy(
            cov.at[pl.ds(32 * i, 32), :],
            ext.at[pl.ds(16 + 32 * i, 32), pl.ds(128, cols)],
            load_sem.at[i],
        )
        copy.start()
        loads.append(copy)
    fog_loads = [
        pltpu.make_async_copy(fogr, fr, fog_sem.at[0]),
        pltpu.make_async_copy(fogc, fc, fog_sem.at[1]),
    ]
    for copy in fog_loads:
        copy.start()

    ext[0:16, :] = jnp.zeros((16, cols + 256), I32)
    ext[272:288, :] = jnp.zeros((16, cols + 256), I32)
    ext[16:272, 0:128] = jnp.zeros((256, 128), I32)
    ext[16:272, cols + 128 : cols + 256] = jnp.zeros((256, 128), I32)
    for buf in (mext, bext):
        buf[0:48, :] = jnp.zeros((48, 128), F32)
        buf[112:160, :] = jnp.zeros((48, 128), F32)

    def at(x, y, c):
        return (stripe, x * SIDE + y, c)

    barrier = pltpu.get_barrier_semaphore()

    def greet(target):
        pl.semaphore_signal(barrier, inc=1, device_id=target, device_id_type=MESH)

    for d in ORDER:
        for c in (0, 1):
            greet(at(px, lax.rem(py + d, SIDE), c))
        greet(at(lax.rem(px + d, SIDE), py, col))
    greet(at(px, py, other))
    crosses_up = jnp.logical_and(py == 0, px > 0)
    crosses_down = jnp.logical_and(py == SIDE - 1, px < SIDE - 1)

    @pl.when(crosses_up)
    def _():
        for c in (0, 1):
            greet((stripe, row - 1, c))

    @pl.when(crosses_down)
    def _():
        for c in (0, 1):
            greet((stripe, row + 1, c))

    for i in range(cols // 256):
        part = (iota((256, 128), 0) + 256 * i) // BS + cells * col
        s1[256 * i : 256 * i + 256, :] = onehot(part == iota((256, 128), 1)).astype(BF16)
    wh, wl = split(taps_of(iota((256, 128), 0) - iota((256, 128), 1) - 64))
    wcat[:, 0:128] = wh
    wcat[:, 128:256] = wl

    for i in range(8):
        loads[i].wait()
        x = ext[16 + 32 * i : 48 + 32 * i, 128 : cols + 128].astype(F32)
        rs[8 * i : 8 * i + 8, :] = x.reshape(4, 8, cols).sum(axis=0)
        cb[16 + 32 * i : 48 + 32 * i, 128 : cols + 128] = x.astype(BF16)
    sums = dot_exact(rs[...], s1[...])
    means = sums.reshape(8, 8, 128).sum(axis=1) * (1.0 / (255.0 * BS * BS))
    mbuf[col, py] = means

    pl.semaphore_wait(
        barrier,
        22 + 2 * crosses_up.astype(I32) + 2 * crosses_down.astype(I32),
    )

    pending = []

    def send(src, dst, s_sem, r_sem, target):
        copy = pltpu.make_async_remote_copy(
            src_ref=src, dst_ref=dst, send_sem=s_sem, recv_sem=r_sem,
            device_id=target, device_id_type=MESH,
        )
        copy.start()
        pending.append((None, copy))

    def send_if(condition, src, dst, s_sem, r_sem, target):
        copy = pltpu.make_async_remote_copy(
            src_ref=src, dst_ref=dst, send_sem=s_sem, recv_sem=r_sem,
            device_id=target, device_id_type=MESH,
        )

        @pl.when(condition)
        def _():
            copy.start()

        pending.append((condition, copy))

    def arrived(dst, r_sem, s_sem):
        pltpu.make_async_remote_copy(
            src_ref=dst, dst_ref=dst, send_sem=s_sem, recv_sem=r_sem,
            device_id=at(px, py, other), device_id_type=MESH,
        ).wait_recv()

    def spread_y(buf, s_sem, r_sem):
        mine = buf.at[col, py]
        slot = r_sem.at[col * SIDE + py]
        for n, d in enumerate(ORDER):
            for c in (0, 1):
                send(mine, mine, s_sem.at[2 * n + c], slot, at(px, lax.rem(py + d, SIDE), c))
        send(mine, mine, s_sem.at[14], slot, at(px, py, other))

    def collect_y(buf, s_sem, r_sem):
        for d in ORDER:
            for c in (0, 1):
                y = lax.rem(py + d, SIDE)
                arrived(buf.at[c, y], r_sem.at[c * SIDE + y], s_sem.at[0])
        arrived(buf.at[other, py], r_sem.at[other * SIDE + py], s_sem.at[0])
        return (buf[0] + buf[1]).reshape(64, 128)

    def spread_x(buf, s_sem, r_sem):
        for n, d in enumerate(ORDER):
            send(buf.at[px], buf.at[px], s_sem.at[n], r_sem.at[px], at(lax.rem(px + d, SIDE), py, col))

    def collect_x(buf, s_sem, r_sem):
        for d in ORDER:
            x = lax.rem(px + d, SIDE)
            arrived(buf.at[x], r_sem.at[x], s_sem.at[0])

    def spread_slabs(buf, s_sem, r_sem):
        send_if(px < SIDE - 1, buf.at[pl.ds(64, 48), :], buf.at[pl.ds(0, 48), :],
                s_sem.at[0], r_sem.at[0], at(px + 1, py, col))
        send_if(px > 0, buf.at[pl.ds(48, 48), :], buf.at[pl.ds(112, 48), :],
                s_sem.at[1], r_sem.at[1], at(px - 1, py, col))

    def collect_slabs(buf, s_sem, r_sem):
        @pl.when(px > 0)
        def _():
            arrived(buf.at[pl.ds(0, 48), :], r_sem.at[0], s_sem.at[0])

        @pl.when(px < SIDE - 1)
        def _():
            arrived(buf.at[pl.ds(112, 48), :], r_sem.at[1], s_sem.at[1])

    spread_y(mbuf, m_send, m_recv)
    own = pl.ds(128, cols)
    inner = pl.ds(pl.multiple_of((1 - col) * (cols - 128) + 128, 128), 128)
    pad_there = pl.ds(pl.multiple_of(col * (cols + 128), 128), 128)
    pad_here = pl.ds(pl.multiple_of(other * (cols + 128), 128), 128)
    body, top, bottom = pl.ds(16, 256), pl.ds(8, 8), pl.ds(272, 8)
    send(ext.at[body, inner], ext.at[body, pad_there], halo_send.at[0], halo_recv.at[0], at(px, py, other))
    up, down = row > 0, row < last
    first8, last8 = pl.ds(16, 8), pl.ds(264, 8)
    send_if(up, ext.at[first8, own], ext.at[bottom, own], halo_send.at[1], halo_recv.at[1], (stripe, row - 1, col))
    send_if(down, ext.at[last8, own], ext.at[top, own], halo_send.at[2], halo_recv.at[2], (stripe, row + 1, col))
    send_if(up, ext.at[first8, inner], ext.at[bottom, pad_there], halo_send.at[3], halo_recv.at[3], (stripe, row - 1, other))
    send_if(down, ext.at[last8, inner], ext.at[top, pad_there], halo_send.at[4], halo_recv.at[4], (stripe, row + 1, other))

    for i in range(wide // 128):
        part = (iota((128, 128), 0) + 128 * i - 64) // BS
        lanes = iota((128, 128), 1)
        inside = jnp.logical_and(part >= 0, part < cells)
        s2[128 * i : 128 * i + 128, :] = onehot(
            jnp.logical_and(inside, part + cells * col == lanes)
        ).astype(BF16)
        cell = (iota((128, 128), 1) + 128 * i + cols * col - 64 + 128) // BS - 4
        sps[:, 128 * i : 128 * i + 128] = onehot(cell == iota((128, 128), 0)).astype(BF16)
    bh, bl = split(taps_of(iota((144, 160), 1) - iota((144, 160), 0)))
    b0[0:144, :] = bh
    b0[144:288, :] = bl
    bh, bl = split(taps_of(iota((144, 160), 1) - iota((144, 160), 0) - 16))
    b16[0:144, :] = bh
    b16[144:288, :] = bl

    def blur_across(src_hi, src_lo, dst_hi, dst_lo, first, count, tiles):
        for j in range(tiles):
            wide_part = dot(src_hi[first : first + count, 128 * j : 128 * j + 256], wcat[...])
            part = wide_part[:, 0:128] + wide_part[:, 128:256]
            if src_lo is not None:
                part = part + dot(src_lo[first : first + count, 128 * j : 128 * j + 256], wcat[:, 0:128])
            high, low = split(part)
            dst_hi[first : first + count, 128 * j : 128 * j + 128] = high
            dst_lo[first : first + count, 128 * j : 128 * j + 128] = low

    arrived(ext.at[body, pad_here], halo_recv.at[0], halo_send.at[0])
    for pad in (0, cols + 128):
        cb[16:272, pad : pad + 128] = ext[16:272, pad : pad + 128].astype(F32).astype(BF16)
    blur_across(cb, None, hhi, hlo, 16, 256, wide // 128)

    mx = collect_y(mbuf, m_send, m_recv)
    mext[48:112, :] = mx
    to_region = jnp.where(
        iota((128, 128), 0) // 8 == lax.rem(iota((128, 128), 1), 16), 1.0 / 64.0, 0.0
    ).astype(BF16)
    own_lanes = iota((64, 128), 1) // 16 == iota((64, 128), 0) // 8

    def region_row(field):
        return jnp.where(own_lanes, dot_exact(field, to_region), 0.0).sum(axis=0, keepdims=True)

    pbuf[px] = region_row(mx)
    spread_slabs(mext, ms_send, ms_recv)
    spread_x(pbuf, p_send, p_recv)

    @pl.when(up)
    def _():
        arrived(ext.at[top, own], halo_recv.at[2], halo_send.at[2])
        arrived(ext.at[top, pad_here], halo_recv.at[4], halo_send.at[4])

    @pl.when(down)
    def _():
        arrived(ext.at[bottom, own], halo_recv.at[1], halo_send.at[1])
        arrived(ext.at[bottom, pad_here], halo_recv.at[3], halo_send.at[3])

    for first in (0, 272):
        cb[first : first + 16, :] = ext[first : first + 16, :].astype(F32).astype(BF16)
        blur_across(cb, None, hhi, hlo, first, 16, wide // 128)

    half = iota((288, 128), 1) < 64
    turned = pltpu.roll(ext[:, 0:128].astype(F32), 64, 1)
    for j in range(wide // 128):
        following = pltpu.roll(ext[:, 128 * j + 128 : 128 * j + 256].astype(F32), 64, 1)
        cs[:, 128 * j : 128 * j + 128] = jnp.where(half, turned, following)
        turned = following

    def blur_down(taps, count, high, low, block, lanes):
        up_part = dot(taps[...] if count == 144 else jnp.concatenate([taps[0:128, :], taps[144:272, :]], 0),
                      high[128 * block : 128 * block + 160, lanes])
        return up_part[0:count] + up_part[count:] + dot(taps[0:count, :], low[128 * block : 128 * block + 160, lanes])

    tiles = [slice(256 * j, 256 * j + 256) for j in range(wide // 256)]
    if wide % 256:
        tiles.append(slice(wide - 128, wide))
    for lanes in tiles:
        for block, taps in ((0, b0), (1, b16)):
            t = 1.5 - blur_down(taps, 144, hhi, hlo, block, lanes) * (0.5 / 255.0)
            tt[144 * block : 144 * block + 144, lanes] = t
            kept = slice(16, 144) if block == 0 else slice(0, 128)
            product = cs[16 + 128 * block : 144 + 128 * block, lanes] * t[kept]
            width = lanes.stop - lanes.start
            asum[32 * block : 32 * block + 32, lanes] = (
                product.reshape(4, 4, 8, width).sum(axis=1).reshape(32, width)
            )
    sums = dot_exact(asum[...], s2[...])
    abuf[col, py] = sums.reshape(8, 8, 128).sum(axis=1) * (1.0 / (255.0 * BS * BS))
    spread_y(abuf, a_send, a_recv)

    across = gauss_of(iota((128, 128), 0) - iota((128, 128), 1))
    across = jnp.where(
        jnp.logical_and(iota((128, 128), 0) < 2 * cells, iota((128, 128), 1) < 2 * cells), across, 0.0
    )
    ah, al = split(across)

    def dot_across(field):
        fh, fl = split(field)
        return dot(fh, ah) + (dot(fl, ah) + dot(fh, al))

    collect_slabs(mext, ms_send, ms_recv)
    swept = dot_across(mext[...])
    back_x = dot3(gauss_of(iota((64, 160), 0) - iota((64, 160), 1) + 48), swept)
    back_24 = dot3(gauss_of(iota((24, 160), 0) - iota((24, 160), 1) + 40 + 8 * py), swept)

    ax = collect_y(abuf, a_send, a_recv)
    bx = ax - 0.3 * back_x * mext[48:112, :]
    bext[48:112, :] = bx
    ebuf[px] = region_row(bx)
    spread_x(ebuf, e_send, e_recv)
    spread_slabs(bext, bs_send, bs_recv)

    for copy in fog_loads:
        copy.wait()
    kr = fr[...]
    kr = kr / jnp.sum(kr, axis=1, keepdims=True)
    kc = fc[...]
    kc = kc / jnp.sum(kc, axis=1, keepdims=True)
    nreg = 2 * cells // 8
    pick = onehot(lax.rem(iota((128, nreg), 0), 16) == iota((128, nreg), 1))
    kct = kc.T
    to_cells = dot_exact(kct, onehot(iota((nreg, 128), 1) // 8 == iota((nreg, 128), 0)))
    to_lanes = dot_exact(kct, onehot(lax.rem(iota((nreg, 128), 1), 16) == iota((nreg, 128), 0)))
    zc = exact_dot(pick, to_cells)
    zl = exact_dot(pick, to_lanes)
    own_kr = jnp.where(iota((64, 64), 0) == row, kr, 0.0).sum(axis=0, keepdims=True)
    own_kr = jnp.where(iota((8, 64), 1) // 8 == iota((8, 64), 0), own_kr, 0.0)
    own_kr = dot_exact(own_kr, onehot(lax.rem(iota((64, 128), 0), 8) == iota((64, 128), 1) // 16))
    collect_x(pbuf, p_send, p_recv)
    regions = pbuf[...]
    spread = jnp.broadcast_to(regions, (8, 8, 128)).reshape(64, 128)
    in_block = iota((64, 128), 1) // 16 == lax.rem(iota((64, 128), 0), 8)
    spread = jnp.where(in_block, spread, 0.0)
    fog_cells = dot3(kr, dot3(spread, zc))
    fog_lanes = dot3(kr, dot3(spread, zl))
    fog_lanes = jnp.where(in_block, fog_lanes, 0.0).reshape(8, 8, 128).sum(axis=1)
    fog_24 = exact_dot(onehot(row - 1 + iota((24, 64), 0) // 8 == iota((24, 64), 1)), fog_cells)
    fog_160 = exact_dot(onehot(8 * px - 6 + iota((160, 64), 0) // 8 == iota((160, 64), 1)), fog_cells)

    coarse = 0.3 * back_24 + 0.2 * fog_24
    row24[...] = dot_exact(coarse, sps[...])
    for first, count, place in [(0, 16, 7)] + [(16 + 32 * i, 32, 8 + i) for i in range(8)] + [(272, 16, 16)]:
        here = slice(first, first + count)
        dose = tt[here, :] - row24[place : place + 1, :]
        tt[here, :] = dose
        high, low = split(cs[here, :] * dose)
        qhi[here, :] = high
        qlo[here, :] = low
    blur_across(qhi, qlo, h2hi, h2lo, 0, 288, cols // 128)
    left = iota((128, 128), 1) < 64
    for j in range(cols // 256):
        lanes = slice(256 * j, 256 * j + 256)
        for block in (0, 1):
            fine = blur_down(b16, 128, h2hi, h2lo, block, lanes)
            here = slice(16 + 128 * block, 144 + 128 * block)
            turned = [pltpu.roll(tt[here, 256 * j + 128 * i : 256 * j + 128 * i + 128], 64, 1) for i in range(3)]
            for i in (0, 1):
                dose = jnp.where(left, turned[i], turned[i + 1])
                x_out[128 * block : 128 * block + 128, 256 * j + 128 * i : 256 * j + 128 * i + 128] = (
                    dose + 0.5 - fine[:, 128 * i : 128 * i + 128] * (0.5 / 255.0)
                )

    collect_slabs(bext, bs_send, bs_recv)
    means2 = bext[...] - 0.2 * fog_160 * mext[...]
    back2 = dot3(gauss_of(iota((8, 160), 0) - iota((8, 160), 1) + 48 + 8 * py), dot_across(means2))
    collect_x(ebuf, e_send, e_recv)
    fog_mean2 = ebuf[...].reshape(8, 128) - 0.2 * fog_lanes * regions.reshape(8, 128)
    weighted = jnp.broadcast_to((own_kr * fog_mean2).sum(axis=0, keepdims=True), (8, 128))
    coarse2 = 0.3 * back2 + 0.2 * dot3(weighted, zc)
    coarse_out[...] = dot_exact(coarse2, sps[:, 64 : cols + 64])

    for condition, copy in pending:
        if condition is None:
            copy.wait_send()
        else:
            pl.when(condition)(copy.wait_send)


def finish_kernel(x, coarse, out, buf, sem):
    cols = coarse.shape[1]
    copies = []
    for i in range(8):
        here = pl.ds(32 * i, 32)
        buf[32 * i : 32 * i + 32, :] = x[32 * i : 32 * i + 32, :] - coarse[i : i + 1, :]
        copy = pltpu.make_async_copy(buf.at[here, :], out.at[here, :], sem.at[i])
        copy.start()
        copies.append(copy)
    for copy in copies:
        copy.wait()


def shards(coverage, fog_rows, fog_cols):
    rows, cols = coverage.shape
    wide = cols + 128
    dma = pltpu.SemaphoreType.DMA
    hbm = pl.BlockSpec(memory_space=pl.ANY)
    vmem = pl.BlockSpec(memory_space=pltpu.VMEM)
    x, coarse = pl.pallas_call(
        correct_kernel,
        out_shape=(
            jax.ShapeDtypeStruct((rows, cols), F32),
            jax.ShapeDtypeStruct((8, cols), F32),
        ),
        in_specs=[hbm, hbm, hbm],
        out_specs=(vmem, vmem),
        scratch_shapes=[
            pltpu.VMEM((288, cols + 256), I32),
            pltpu.VMEM((288, cols + 256), BF16),
            pltpu.VMEM((64, cols), F32),
            pltpu.VMEM((288, wide), F32),
            pltpu.VMEM((288, wide), BF16),
            pltpu.VMEM((288, wide), BF16),
            pltpu.VMEM((288, wide), F32),
            pltpu.VMEM((64, wide), F32),
            pltpu.VMEM((288, wide), BF16),
            pltpu.VMEM((288, wide), BF16),
            pltpu.VMEM((288, cols), BF16),
            pltpu.VMEM((288, cols), BF16),
            pltpu.VMEM((cols, 128), BF16),
            pltpu.VMEM((wide, 128), BF16),
            pltpu.VMEM((128, wide), BF16),
            pltpu.VMEM((256, 256), BF16),
            pltpu.VMEM((288, 160), BF16),
            pltpu.VMEM((288, 160), BF16),
            pltpu.VMEM((24, wide), F32),
            pltpu.VMEM((2, SIDE, 8, 128), F32),
            pltpu.VMEM((160, 128), F32),
            pltpu.VMEM((SIDE, 1, 128), F32),
            pltpu.VMEM((2, SIDE, 8, 128), F32),
            pltpu.VMEM((160, 128), F32),
            pltpu.VMEM((SIDE, 1, 128), F32),
            pltpu.VMEM(fog_rows.shape, F32),
            pltpu.VMEM(fog_cols.shape, F32),
            dma((8,)), dma((2,)), dma((5,)), dma((5,)),
            dma((16,)), dma((16,)), dma((16,)), dma((16,)),
            dma((8,)), dma((8,)), dma((8,)), dma((8,)),
            dma((2,)), dma((2,)), dma((2,)), dma((2,)),
        ],
        compiler_params=pltpu.CompilerParams(
            collective_id=0, has_side_effects=True, vmem_limit_bytes=44 * 1024 * 1024
        ),
    )(coverage, fog_rows, fog_cols)
    return pl.pallas_call(
        finish_kernel,
        out_shape=jax.ShapeDtypeStruct((rows, cols), F32),
        in_specs=[vmem, vmem],
        out_specs=hbm,
        scratch_shapes=[pltpu.VMEM((rows, cols), F32), dma((8,))],
        compiler_params=pltpu.CompilerParams(vmem_limit_bytes=8 * 1024 * 1024),
    )(x, coarse)


def solution(mesh):
    placed = (P(("stripe", "row"), "col"), P(), P())
    return jax.shard_map(
        shards, mesh=mesh, in_specs=placed, out_specs=P(("stripe", "row"), "col"), check_vma=False
    )
```

```python
import math

import jax
import jax.numpy as jnp
from jax import lax
from jax.experimental import pallas as pl
from jax.experimental.pallas import tpu as pltpu
from jax.sharding import PartitionSpec as P

BS = 32
FB = 256
HALO = 4
BSIG = 16
REACH = 40
SIDE = 8
MESH = pl.DeviceIdType.MESH
F32 = jnp.float32
BF16 = jnp.bfloat16
I32 = jnp.int32
ORDER = (4, 3, 5, 2, 6, 1, 7)

TAPS = [math.exp(-(k * k) / (2 * 1.25**2)) for k in range(-HALO, HALO + 1)]
TAP_SCALE = 1.0 / sum(TAPS)
GAUSS_SCALE = 1.0 / (BSIG * math.sqrt(2.0 * math.pi))


def iota(shape, dim):
    return lax.broadcasted_iota(I32, shape, dim)


def onehot(condition):
    return jnp.where(condition, 1.0, 0.0).astype(F32)


def taps_of(offset):
    square = (offset * offset).astype(F32)
    value = jnp.exp(square * (-1.0 / (2 * 1.25**2))) * TAP_SCALE
    return jnp.where(jnp.abs(offset) <= HALO, value, 0.0)


def gauss_of(offset):
    square = (offset * offset).astype(F32)
    value = jnp.exp(square * (-0.5 / (BSIG * BSIG))) * GAUSS_SCALE
    return jnp.where(jnp.abs(offset) <= REACH, value, 0.0)


def split(value):
    high = value.astype(BF16)
    return high, (value - high.astype(F32)).astype(BF16)


def dot(a, b):
    return jnp.dot(a, b, preferred_element_type=F32)


def dot_exact(a, b):
    high, low = split(a)
    b = b.astype(BF16)
    return dot(high, b) + dot(low, b)


def exact_dot(a, b):
    high, low = split(b)
    a = a.astype(BF16)
    return dot(a, high) + dot(a, low)


def dot3(a, b):
    ah, al = split(a)
    bh, bl = split(b)
    return dot(ah, bh) + (dot(al, bh) + dot(ah, bl))


def correct_kernel(
    cov, fogr, fogc, x_out, coarse_out,
    ext, cb, rs, cs, hhi, hlo, tt, asum, qhi, qlo, h2hi, h2lo,
    s1, s2, sps, wcat, b16, zp, row24, mbuf, mext, pbuf, abuf, bext, ebuf, fr, fc,
    edge_sem, load_sem, fog_sem, halo_send, halo_recv, ready,
    m_sem, a_sem, p_sem, e_sem, ms_sem, bs_sem,
):
    stripe = lax.axis_index("stripe")
    row = lax.axis_index("row")
    col = lax.axis_index("col")
    px = row // SIDE
    py = lax.rem(row, SIDE)
    other = 1 - col
    rows, cols = 256, cov.shape[1]
    cells = cols // BS
    wide = cols + 128
    last = SIDE * SIDE - 1
    mine = col * SIDE + py

    own = pl.ds(128, cols)
    first8, last8 = pl.ds(16, 8), pl.ds(264, 8)
    for at_row in (0, 248):
        pltpu.make_async_copy(
            cov.at[pl.ds(at_row, 8), :], ext.at[pl.ds(16 + at_row, 8), own], edge_sem
        ).start()
    spans = [(8, 32), (32, 64), (64, 96), (96, 128), (128, 160), (160, 192), (192, 224), (224, 248)]
    for i, (start, stop) in enumerate(spans):
        pltpu.make_async_copy(
            cov.at[pl.ds(start, stop - start), :],
            ext.at[pl.ds(16 + start, stop - start), own],
            load_sem.at[i // 2],
        ).start()
    fog_loads = [
        pltpu.make_async_copy(fogr, fr, fog_sem.at[0]),
        pltpu.make_async_copy(fogc, fc, fog_sem.at[1]),
    ]
    for copy in fog_loads:
        copy.start()

    def whole(ref, sem):
        pltpu.make_async_copy(ref, ref, sem).wait()

    ext[0:16, :] = jnp.zeros((16, cols + 256), I32)
    ext[272:288, :] = jnp.zeros((16, cols + 256), I32)
    ext[16:272, 0:128] = jnp.zeros((256, 128), I32)
    ext[16:272, cols + 128 : cols + 256] = jnp.zeros((256, 128), I32)
    for buf in (mext, bext):
        buf[0:48, :] = jnp.zeros((48, 128), F32)
        buf[112:160, :] = jnp.zeros((48, 128), F32)

    def at(x, y, c):
        return (stripe, x * SIDE + y, c)

    def beside_y(d):
        return lax.rem(py + d, SIDE)

    def beside_x(d):
        return lax.rem(px + d, SIDE)

    barrier = pltpu.get_barrier_semaphore()

    def signal(sem, target):
        pl.semaphore_signal(sem, inc=1, device_id=target, device_id_type=MESH)

    crosses_up = jnp.logical_and(py == 0, px > 0)
    crosses_down = jnp.logical_and(py == SIDE - 1, px < SIDE - 1)
    for d in (1, 7):
        for c in (0, 1):
            signal(barrier, at(px, beside_y(d), c))
        signal(barrier, at(beside_x(d), py, col))
    signal(barrier, at(px, py, other))

    @pl.when(crosses_up)
    def _():
        for c in (0, 1):
            signal(barrier, (stripe, row - 1, c))

    @pl.when(crosses_down)
    def _():
        for c in (0, 1):
            signal(barrier, (stripe, row + 1, c))

    def send(src, dst, s_sem, r_sem, target):
        pltpu.make_async_remote_copy(
            src_ref=src, dst_ref=dst, send_sem=s_sem, recv_sem=r_sem,
            device_id=target, device_id_type=MESH,
        ).start()

    inner = pl.ds(pl.multiple_of((1 - col) * (cols - 128) + 128, 128), 128)
    pad_there = pl.ds(pl.multiple_of(col * (cols + 128), 128), 128)
    pad_here = pl.ds(pl.multiple_of(other * (cols + 128), 128), 128)
    body, top, bottom = pl.ds(16, 256), pl.ds(8, 8), pl.ds(272, 8)
    both = pl.ds(0, cols + 128)
    up, down = row > 0, row < last

    whole(ext.at[pl.ds(16, 16), own], edge_sem)
    pl.semaphore_wait(
        barrier,
        7 + 2 * crosses_up.astype(I32) + 2 * crosses_down.astype(I32),
    )

    @pl.when(up)
    def _():
        send(ext.at[first8, own], ext.at[bottom, own], halo_send.at[1], halo_recv.at[1], (stripe, row - 1, col))
        send(ext.at[first8, inner], ext.at[bottom, pad_there], halo_send.at[1], halo_recv.at[1], (stripe, row - 1, other))

    @pl.when(down)
    def _():
        send(ext.at[last8, own], ext.at[top, own], halo_send.at[2], halo_recv.at[2], (stripe, row + 1, col))
        send(ext.at[last8, inner], ext.at[top, pad_there], halo_send.at[2], halo_recv.at[2], (stripe, row + 1, other))

    for d in (1, 7):
        signal(ready.at[0], at(px, beside_y(d), col))
        signal(ready.at[0], at(beside_x(d), py, col))

    for i in range(cols // 256):
        part = (iota((256, 128), 0) + 256 * i) // BS + cells * col
        s1[256 * i : 256 * i + 256, :] = onehot(part == iota((256, 128), 1)).astype(BF16)
    wh, wl = split(taps_of(iota((256, 128), 0) - iota((256, 128), 1) - 64))
    wcat[:, 0:128] = wh
    wcat[:, 128:256] = wl
    bh, bl = split(taps_of(iota((144, 160), 1) - iota((144, 160), 0) - 16))
    b16[0:144, :] = bh
    b16[144:288, :] = bl
    for i in range(wide // 128):
        part = (iota((128, 128), 0) + 128 * i - 64) // BS
        inside = jnp.logical_and(part >= 0, part < cells)
        s2[128 * i : 128 * i + 128, :] = onehot(
            jnp.logical_and(inside, part + cells * col == iota((128, 128), 1))
        ).astype(BF16)

    for i in range(8):
        if i % 2 == 0:
            start = spans[i][0]
            whole(ext.at[pl.ds(16 + start, spans[i + 1][1] - start), own], load_sem.at[i // 2])
        x = ext[16 + 32 * i : 48 + 32 * i, 128 : cols + 128].astype(F32)
        rs[8 * i : 8 * i + 8, :] = x.reshape(4, 8, cols).sum(axis=0)
        cb[16 + 32 * i : 48 + 32 * i, 128 : cols + 128] = x.astype(BF16)
    sums = dot_exact(rs[...], s1[...])
    means = sums.reshape(8, 8, 128).sum(axis=1) * (1.0 / (255.0 * BS * BS))
    mbuf[mine] = means

    send(ext.at[body, inner], ext.at[body, pad_there], halo_send.at[0], halo_recv.at[0], at(px, py, other))

    pl.semaphore_wait(ready.at[0], 4)
    for d in (2, 6):
        signal(ready.at[1], at(px, beside_y(d), col))
        signal(ready.at[1], at(beside_x(d), py, col))

    def spread_y(buf, sem):
        for d in ORDER:
            for c in (0, 1):
                send(buf.at[mine], buf.at[mine], sem.at[0], sem.at[1], at(px, beside_y(d), c))
        send(buf.at[mine], buf.at[mine], sem.at[0], sem.at[1], at(px, py, other))

    def collect_y(buf, sem):
        whole(buf.at[pl.ds(0, 2 * SIDE - 1)], sem.at[1])
        return (buf[0:SIDE] + buf[SIDE:]).reshape(64, 128)

    def spread_x(buf, sem):
        for d in ORDER:
            send(buf.at[px], buf.at[px], sem.at[0], sem.at[1], at(beside_x(d), py, col))

    def collect_x(buf, sem):
        whole(buf.at[pl.ds(0, SIDE - 1)], sem.at[1])

    def spread_slabs(buf, sem):
        @pl.when(px < SIDE - 1)
        def _():
            send(buf.at[pl.ds(64, 48), :], buf.at[pl.ds(0, 48), :],
                 sem.at[0], sem.at[2], at(px + 1, py, col))

        @pl.when(px > 0)
        def _():
            send(buf.at[pl.ds(48, 48), :], buf.at[pl.ds(112, 48), :],
                 sem.at[1], sem.at[3], at(px - 1, py, col))

    def collect_slabs(buf, sem):
        @pl.when(px > 0)
        def _():
            whole(buf.at[pl.ds(0, 48), :], sem.at[2])

        @pl.when(px < SIDE - 1)
        def _():
            whole(buf.at[pl.ds(112, 48), :], sem.at[3])

    def pieces(ref, parts, lanes):
        found = [ref[first : first + count, lanes] for first, count in parts]
        return found[0] if len(found) == 1 else jnp.concatenate(found, axis=0)

    def put(ref, parts, lanes, value):
        at_row = 0
        for first, count in parts:
            ref[first : first + count, lanes] = value[at_row : at_row + count]
            at_row += count

    def blur_across(src_hi, src_lo, dst_hi, dst_lo, parts, tiles):
        for j in range(tiles):
            window, lanes = slice(128 * j, 128 * j + 256), slice(128 * j, 128 * j + 128)
            wide_part = dot(pieces(src_hi, parts, window), wcat[...])
            part = wide_part[:, 0:128] + wide_part[:, 128:256]
            if src_lo is not None:
                part = part + dot(pieces(src_lo, parts, window), wcat[:, 0:128])
            high, low = split(part)
            put(dst_hi, parts, lanes, high)
            put(dst_lo, parts, lanes, low)

    def shift_coverage(parts):
        count = sum(n for _, n in parts)
        half = iota((count, 128), 1) < 64
        turned = pltpu.roll(pieces(ext, parts, slice(0, 128)).astype(F32), 64, 1)
        for j in range(wide // 128):
            following = pieces(ext, parts, slice(128 * j + 128, 128 * j + 256)).astype(F32)
            following = pltpu.roll(following, 64, 1)
            put(cs, parts, slice(128 * j, 128 * j + 128), jnp.where(half, turned, following))
            turned = following

    def blur_down(count, depth, high, low, first, lanes):
        both = jnp.concatenate([b16[0:count, 0:depth], b16[144 : 144 + count, 0:depth]], 0)
        here = slice(first, first + depth)
        result = dot(both, high[here, lanes])
        return result[0:count] + result[count:] + dot(b16[0:count, 0:depth], low[here, lanes])

    body_rows, edge_rows = ((16, 256),), ((0, 16), (272, 16))
    whole(ext.at[body, pad_here], halo_recv.at[0])
    for pad in (0, cols + 128):
        cb[16:272, pad : pad + 128] = ext[16:272, pad : pad + 128].astype(F32).astype(BF16)
    blur_across(cb, None, hhi, hlo, body_rows, wide // 128)
    shift_coverage(body_rows)

    tiles = [slice(256 * j, 256 * j + 256) for j in range(wide // 256)]
    if wide % 256:
        tiles.append(slice(wide - 128, wide))

    def main_rows(lanes):
        width = lanes.stop - lanes.start
        for block in (0, 1):
            here = slice(32 + 112 * block, 144 + 112 * block)
            t = 1.5 - blur_down(112, 144, hhi, hlo, 16 + 112 * block, lanes) * (0.5 / 255.0)
            tt[here, lanes] = t
            product = cs[here, lanes] * t
            whole = product[16:112] if block == 0 else product[0:96]
            half = product[0:16] if block == 0 else product[96:112]
            whole = whole.reshape(3, 4, 8, width).sum(axis=1).reshape(24, width)
            asum[8 + 24 * block : 32 + 24 * block, lanes] = whole
            asum[56 * block : 56 * block + 8, lanes] = half[0:8] + half[8:16]

    for lanes in tiles:
        main_rows(lanes)

    pl.semaphore_wait(ready.at[1], 4)
    spread_y(mbuf, m_sem)

    for i in range(wide // 128):
        cell = (iota((128, 128), 1) + 128 * i + cols * col - 64 + 128) // BS - 4
        sps[:, 128 * i : 128 * i + 128] = onehot(cell == iota((128, 128), 0)).astype(BF16)

    to_region = jnp.where(
        iota((128, 128), 0) // 8 == lax.rem(iota((128, 128), 1), 16), 1.0 / 64.0, 0.0
    ).astype(BF16)
    own_lanes = iota((64, 128), 1) // 16 == iota((64, 128), 0) // 8

    def region_row(field):
        return jnp.where(own_lanes, dot_exact(field, to_region), 0.0).sum(axis=0, keepdims=True)

    across = gauss_of(iota((128, 128), 0) - iota((128, 128), 1))
    across = jnp.where(
        jnp.logical_and(iota((128, 128), 0) < 2 * cells, iota((128, 128), 1) < 2 * cells), across, 0.0
    )
    ah, al = split(across)

    def dot_across(field):
        fh, fl = split(field)
        return dot(fh, ah) + (dot(fl, ah) + dot(fh, al))

    for copy in fog_loads:
        copy.wait()
    kr = fr[...]
    kr = kr / jnp.sum(kr, axis=1, keepdims=True)
    kc = fc[...]
    kc = kc / jnp.sum(kc, axis=1, keepdims=True)
    nreg = 2 * cells // 8
    pick = onehot(lax.rem(iota((128, nreg), 0), 16) == iota((128, nreg), 1))
    kct = kc.T
    to_cells = dot_exact(kct, onehot(iota((nreg, 128), 1) // 8 == iota((nreg, 128), 0)))
    to_lanes = dot_exact(kct, onehot(lax.rem(iota((nreg, 128), 1), 16) == iota((nreg, 128), 0)))
    zc = exact_dot(pick, to_cells)
    zl = exact_dot(pick, to_lanes)
    zboth = jnp.concatenate([zc, zl], axis=1)
    in_block = iota((64, 128), 1) // 16 == lax.rem(iota((64, 128), 0), 8)
    kr_24 = exact_dot(onehot(row - 1 + iota((24, 64), 0) // 8 == iota((24, 64), 1)), kr)
    kr_160 = exact_dot(onehot(8 * px - 6 + iota((160, 64), 0) // 8 == iota((160, 64), 1)), kr)
    own_kr = jnp.where(iota((64, 64), 0) == row, kr, 0.0).sum(axis=0, keepdims=True)
    own_kr = jnp.where(iota((8, 64), 1) // 8 == iota((8, 64), 0), own_kr, 0.0)
    own_kr = dot_exact(own_kr, onehot(lax.rem(iota((64, 128), 0), 8) == iota((64, 128), 1) // 16))
    zph, zpl = split(dot_exact(0.2 * zc, sps[:, 64 : cols + 64]))
    zp[0] = zph
    zp[1] = zpl
    part, side = iota((128, 192), 0) // 64, lax.rem(iota((128, 192), 0) // 32, 2)
    piece = iota((128, 192), 1) // 48
    value = taps_of(lax.rem(iota((128, 192), 1), 48) - lax.rem(iota((128, 192), 0), 32) - 16 * side)
    high, low = split(value)
    value = jnp.where(part == 0, high.astype(F32), jnp.where(lax.rem(piece, 2) == 0, low.astype(F32), 0.0))
    edge_taps = jnp.where(side == piece // 2, value, 0.0).astype(BF16)


    @pl.when(up)
    def _():
        whole(ext.at[top, both], halo_recv.at[2])

    @pl.when(down)
    def _():
        whole(ext.at[bottom, both], halo_recv.at[1])

    for first in (0, 272):
        cb[first : first + 16, :] = ext[first : first + 16, :].astype(F32).astype(BF16)
    blur_across(cb, None, hhi, hlo, edge_rows, wide // 128)
    shift_coverage(edge_rows)
    for lanes in tiles:
        inputs = jnp.concatenate(
            [hhi[0:48, lanes], hlo[0:48, lanes], hhi[240:288, lanes], hlo[240:288, lanes]], 0
        )
        result = dot(edge_taps, inputs)
        t = 1.5 - (result[0:64] + result[64:128]) * (0.5 / 255.0)
        tt[0:32, lanes] = t[0:32]
        tt[256:288, lanes] = t[32:64]
        product = cs[16:32, lanes] * t[16:32]
        asum[64:72, lanes] = product[0:8] + product[8:16]
        product = cs[256:272, lanes] * t[32:48]
        asum[72:80, lanes] = product[0:8] + product[8:16]
    sums = dot_exact(asum[...], s2[...]).reshape(10, 8, 128).sum(axis=1)
    cell_row = iota((8, 128), 0)
    sums = (
        sums[0:8]
        + jnp.where(cell_row == 0, sums[8:9], 0.0)
        + jnp.where(cell_row == 7, sums[9:10], 0.0)
    )
    abuf[mine] = sums * (1.0 / (255.0 * BS * BS))
    spread_y(abuf, a_sem)

    mx = collect_y(mbuf, m_sem)
    mext[48:112, :] = mx
    pbuf[px] = region_row(mx)
    spread_x(pbuf, p_sem)
    spread_slabs(mext, ms_sem)
    collect_slabs(mext, ms_sem)
    swept = dot_across(mext[...])
    back_x = dot3(gauss_of(iota((64, 160), 0) - iota((64, 160), 1) + 48), swept)
    back_24 = dot3(gauss_of(iota((24, 160), 0) - iota((24, 160), 1) + 40 + 8 * py), swept)

    ax = collect_y(abuf, a_sem)
    bx = ax - 0.3 * back_x * mext[48:112, :]
    bext[48:112, :] = bx
    ebuf[px] = region_row(bx)
    spread_x(ebuf, e_sem)
    spread_slabs(bext, bs_sem)

    collect_x(pbuf, p_sem)
    regions = pbuf[...]
    spread = jnp.broadcast_to(regions, (8, 8, 128)).reshape(64, 128)
    fog_wide = dot3(jnp.where(in_block, spread, 0.0), zboth)
    fog_24 = dot3(kr_24, fog_wide[:, 0:128])

    coarse = 0.3 * back_24 + 0.2 * fog_24
    row24[...] = dot_exact(coarse, sps[...])
    fog_lanes = jnp.where(in_block, dot3(kr, fog_wide[:, 128:256]), 0.0).reshape(8, 8, 128).sum(axis=1)
    fog_160 = dot3(kr_160, fog_wide[:, 0:128])
    for first, count, place in [(0, 16, 7)] + [(16 + 32 * i, 32, 8 + i) for i in range(8)] + [(272, 16, 16)]:
        here = slice(first, first + count)
        dose = tt[here, :] - row24[place : place + 1, :]
        tt[here, :] = dose
        high, low = split(cs[here, :] * dose)
        qhi[here, :] = high
        qlo[here, :] = low
    blur_across(qhi, qlo, h2hi, h2lo, ((0, 288),), cols // 128)
    left = iota((128, 128), 1) < 64
    for j in range(cols // 256):
        lanes = slice(256 * j, 256 * j + 256)
        for block in (0, 1):
            fine = blur_down(128, 160, h2hi, h2lo, 128 * block, lanes)
            here = slice(16 + 128 * block, 144 + 128 * block)
            turned = [pltpu.roll(tt[here, 256 * j + 128 * i : 256 * j + 128 * i + 128], 64, 1) for i in range(3)]
            for i in (0, 1):
                dose = jnp.where(left, turned[i], turned[i + 1])
                x_out[128 * block : 128 * block + 128, 256 * j + 128 * i : 256 * j + 128 * i + 128] = (
                    dose + 0.5 - fine[:, 128 * i : 128 * i + 128] * (0.5 / 255.0)
                )

    whole(mbuf.at[pl.ds(0, 2 * SIDE - 1)], m_sem.at[0])
    whole(abuf.at[pl.ds(0, 2 * SIDE - 1)], a_sem.at[0])
    whole(pbuf.at[pl.ds(0, SIDE - 1)], p_sem.at[0])
    whole(ebuf.at[pl.ds(0, SIDE - 1)], e_sem.at[0])
    whole(ext.at[body, pad_here], halo_send.at[0])

    @pl.when(up)
    def _():
        whole(ext.at[top, both], halo_send.at[1])

    @pl.when(down)
    def _():
        whole(ext.at[bottom, both], halo_send.at[2])

    for sem in (ms_sem, bs_sem):
        @pl.when(px < SIDE - 1)
        def _():
            whole(mext.at[pl.ds(0, 48), :], sem.at[0])

        @pl.when(px > 0)
        def _():
            whole(mext.at[pl.ds(112, 48), :], sem.at[1])

    collect_slabs(bext, bs_sem)
    means2 = bext[...] - 0.2 * fog_160 * mext[...]
    back2 = dot3(gauss_of(iota((8, 160), 0) - iota((8, 160), 1) + 48 + 8 * py), dot_across(means2))
    coarse_out[...] = dot_exact(0.3 * back2, sps[:, 64 : cols + 64])
    fog_known = 0.2 * fog_lanes * regions.reshape(8, 128)
    collect_x(ebuf, e_sem)
    fog_mean2 = ebuf[...].reshape(8, 128) - fog_known
    weighted = jnp.broadcast_to((own_kr * fog_mean2).sum(axis=0, keepdims=True), (8, 128))
    high, low = split(weighted)
    fog2 = dot(high, zp[0]) + (dot(low, zp[0]) + dot(high, zp[1]))
    coarse_out[...] = coarse_out[...] + fog2


def finish_kernel(x, coarse, out, buf, sem):
    cols = coarse.shape[1]
    copies = []
    for i in range(8):
        here = pl.ds(32 * i, 32)
        buf[32 * i : 32 * i + 32, :] = x[32 * i : 32 * i + 32, :] - coarse[i : i + 1, :]
        copy = pltpu.make_async_copy(buf.at[here, :], out.at[here, :], sem.at[i])
        copy.start()
        copies.append(copy)
    for copy in copies:
        copy.wait()


def shards(coverage, fog_rows, fog_cols):
    rows, cols = coverage.shape
    wide = cols + 128
    dma = pltpu.SemaphoreType.DMA
    hbm = pl.BlockSpec(memory_space=pl.ANY)
    vmem = pl.BlockSpec(memory_space=pltpu.VMEM)
    x, coarse = pl.pallas_call(
        correct_kernel,
        out_shape=(
            jax.ShapeDtypeStruct((rows, cols), F32),
            jax.ShapeDtypeStruct((8, cols), F32),
        ),
        in_specs=[pl.BlockSpec(memory_space=pltpu.MemorySpace.HBM)] * 3,
        out_specs=(vmem, vmem),
        scratch_shapes=[
            pltpu.VMEM((288, cols + 256), I32),
            pltpu.VMEM((288, cols + 256), BF16),
            pltpu.VMEM((64, cols), F32),
            pltpu.VMEM((288, wide), F32),
            pltpu.VMEM((288, wide), BF16),
            pltpu.VMEM((288, wide), BF16),
            pltpu.VMEM((288, wide), F32),
            pltpu.VMEM((80, wide), F32),
            pltpu.VMEM((288, wide), BF16),
            pltpu.VMEM((288, wide), BF16),
            pltpu.VMEM((288, cols), BF16),
            pltpu.VMEM((288, cols), BF16),
            pltpu.VMEM((cols, 128), BF16),
            pltpu.VMEM((wide, 128), BF16),
            pltpu.VMEM((128, wide), BF16),
            pltpu.VMEM((256, 256), BF16),
            pltpu.VMEM((288, 160), BF16),
            pltpu.VMEM((2, 128, cols), BF16),
            pltpu.VMEM((24, wide), F32),
            pltpu.VMEM((2 * SIDE, 8, 128), F32),
            pltpu.VMEM((160, 128), F32),
            pltpu.VMEM((SIDE, 1, 128), F32),
            pltpu.VMEM((2 * SIDE, 8, 128), F32),
            pltpu.VMEM((160, 128), F32),
            pltpu.VMEM((SIDE, 1, 128), F32),
            pltpu.VMEM(fog_rows.shape, F32),
            pltpu.VMEM(fog_cols.shape, F32),
            dma(()), dma((4,)), dma((2,)), dma((3,)), dma((3,)), pltpu.SemaphoreType.REGULAR((2,)),
            dma((2,)), dma((2,)), dma((2,)), dma((2,)), dma((4,)), dma((4,)),
        ],
        compiler_params=pltpu.CompilerParams(
            collective_id=0, has_side_effects=True, vmem_limit_bytes=44 * 1024 * 1024
        ),
    )(*[pltpu.with_memory_space_constraint(v, pltpu.MemorySpace.HBM) for v in (coverage, fog_rows, fog_cols)])
    return pl.pallas_call(
        finish_kernel,
        out_shape=jax.ShapeDtypeStruct((rows, cols), F32),
        in_specs=[vmem, vmem],
        out_specs=hbm,
        scratch_shapes=[pltpu.VMEM((rows, cols), F32), dma((8,))],
        compiler_params=pltpu.CompilerParams(vmem_limit_bytes=8 * 1024 * 1024),
    )(x, coarse)


def solution(mesh):
    placed = (P(("stripe", "row"), "col"), P(), P())
    return jax.shard_map(
        shards, mesh=mesh, in_specs=placed, out_specs=P(("stripe", "row"), "col"), check_vma=False
    )
```

```python
import math

import jax
import jax.numpy as jnp
from jax import lax
from jax.experimental import pallas as pl
from jax.experimental.pallas import tpu as pltpu
from jax.sharding import PartitionSpec as P

BS = 32
FB = 256
HALO = 4
BSIG = 16
REACH = 40
SIDE = 8
MESH = pl.DeviceIdType.MESH
F32 = jnp.float32
BF16 = jnp.bfloat16
I32 = jnp.int32
ORDER = (4, 3, 5, 2, 6, 1, 7)

TAPS = [math.exp(-(k * k) / (2 * 1.25**2)) for k in range(-HALO, HALO + 1)]
TAP_SCALE = 1.0 / sum(TAPS)
GAUSS_SCALE = 1.0 / (BSIG * math.sqrt(2.0 * math.pi))


def iota(shape, dim):
    return lax.broadcasted_iota(I32, shape, dim)


def onehot(condition):
    return jnp.where(condition, 1.0, 0.0).astype(F32)


def taps_of(offset):
    square = (offset * offset).astype(F32)
    value = jnp.exp(square * (-1.0 / (2 * 1.25**2))) * TAP_SCALE
    return jnp.where(jnp.abs(offset) <= HALO, value, 0.0)


def gauss_of(offset):
    square = (offset * offset).astype(F32)
    value = jnp.exp(square * (-0.5 / (BSIG * BSIG))) * GAUSS_SCALE
    return jnp.where(jnp.abs(offset) <= REACH, value, 0.0)


def split(value):
    high = value.astype(BF16)
    return high, (value - high.astype(F32)).astype(BF16)


def dot(a, b):
    return jnp.dot(a, b, preferred_element_type=F32)


def dot_exact(a, b):
    high, low = split(a)
    b = b.astype(BF16)
    return dot(high, b) + dot(low, b)


def exact_dot(a, b):
    high, low = split(b)
    a = a.astype(BF16)
    return dot(a, high) + dot(a, low)


def dot3(a, b):
    ah, al = split(a)
    bh, bl = split(b)
    return dot(ah, bh) + (dot(al, bh) + dot(ah, bl))


def packed(tile):
    return tile[0:4] + pltpu.roll(tile, 64, 1)[4:8]


def unpacked(buf):
    left = iota((4, 128), 1) < 64
    parts = []
    for y in range(SIDE):
        first, second = buf[y], buf[SIDE + y]
        parts.append(jnp.where(left, first, pltpu.roll(second, 64, 1)))
        parts.append(jnp.where(left, pltpu.roll(first, 64, 1), second))
    return jnp.concatenate(parts, axis=0)


def correct_kernel(
    cov, fogr, fogc, x_out, coarse_out,
    ext, cb, rs, cs, hhi, hlo, tt, asum, qhi, qlo, h2hi, h2lo,
    s1, s2, sps, wcat, b16, zp, row24, mbuf, mext, pbuf, abuf, bext, ebuf, fr, fc,
    edge_sem, load_sem, fog_sem, halo_send, halo_recv, ready,
    m_sem, a_sem, p_sem, e_sem, ms_sem, bs_sem,
):
    stripe = lax.axis_index("stripe")
    row = lax.axis_index("row")
    col = lax.axis_index("col")
    px = row // SIDE
    py = lax.rem(row, SIDE)
    other = 1 - col
    rows, cols = 256, cov.shape[1]
    cells = cols // BS
    wide = cols + 128
    last = SIDE * SIDE - 1
    mine = col * SIDE + py

    own = pl.ds(128, cols)
    first8, last8 = pl.ds(16, 8), pl.ds(264, 8)
    for at_row in (0, 248):
        pltpu.make_async_copy(
            cov.at[pl.ds(at_row, 8), :], ext.at[pl.ds(16 + at_row, 8), own], edge_sem
        ).start()
    spans = [(8, 32), (32, 64), (64, 96), (96, 128), (128, 160), (160, 192), (192, 224), (224, 248)]
    for i, (start, stop) in enumerate(spans):
        pltpu.make_async_copy(
            cov.at[pl.ds(start, stop - start), :],
            ext.at[pl.ds(16 + start, stop - start), own],
            load_sem.at[i // 2],
        ).start()
    fog_loads = [
        pltpu.make_async_copy(fogr, fr, fog_sem.at[0]),
        pltpu.make_async_copy(fogc, fc, fog_sem.at[1]),
    ]
    for copy in fog_loads:
        copy.start()

    def whole(ref, sem):
        pltpu.make_async_copy(ref, ref, sem).wait()

    ext[0:16, :] = jnp.zeros((16, cols + 256), I32)
    ext[272:288, :] = jnp.zeros((16, cols + 256), I32)
    ext[16:272, 0:128] = jnp.zeros((256, 128), I32)
    ext[16:272, cols + 128 : cols + 256] = jnp.zeros((256, 128), I32)
    for buf in (mext, bext):
        buf[0:48, :] = jnp.zeros((48, 128), F32)
        buf[112:160, :] = jnp.zeros((48, 128), F32)

    def at(x, y, c):
        return (stripe, x * SIDE + y, c)

    def beside_y(d):
        return lax.rem(py + d, SIDE)

    def beside_x(d):
        return lax.rem(px + d, SIDE)

    barrier = pltpu.get_barrier_semaphore()

    def signal(sem, target):
        pl.semaphore_signal(sem, inc=1, device_id=target, device_id_type=MESH)

    crosses_up = jnp.logical_and(py == 0, px > 0)
    crosses_down = jnp.logical_and(py == SIDE - 1, px < SIDE - 1)
    for d in (1, 7):
        for c in (0, 1):
            signal(barrier, at(px, beside_y(d), c))
        signal(barrier, at(beside_x(d), py, col))
    signal(barrier, at(px, py, other))

    @pl.when(crosses_up)
    def _():
        for c in (0, 1):
            signal(barrier, (stripe, row - 1, c))

    @pl.when(crosses_down)
    def _():
        for c in (0, 1):
            signal(barrier, (stripe, row + 1, c))

    def send(src, dst, s_sem, r_sem, target):
        pltpu.make_async_remote_copy(
            src_ref=src, dst_ref=dst, send_sem=s_sem, recv_sem=r_sem,
            device_id=target, device_id_type=MESH,
        ).start()

    inner = pl.ds(pl.multiple_of((1 - col) * (cols - 128) + 128, 128), 128)
    pad_there = pl.ds(pl.multiple_of(col * (cols + 128), 128), 128)
    pad_here = pl.ds(pl.multiple_of(other * (cols + 128), 128), 128)
    body, top, bottom = pl.ds(16, 256), pl.ds(8, 8), pl.ds(272, 8)
    both = pl.ds(0, cols + 128)
    up, down = row > 0, row < last

    for i in range(cols // 256):
        part = (iota((256, 128), 0) + 256 * i) // BS
        s1[256 * i : 256 * i + 256, :] = onehot(part == iota((256, 128), 1)).astype(BF16)
    wh, wl = split(taps_of(iota((256, 128), 0) - iota((256, 128), 1) - 64))
    wcat[:, 0:128] = wh
    wcat[:, 128:256] = wl
    bh, bl = split(taps_of(iota((144, 160), 1) - iota((144, 160), 0) - 16))
    b16[0:144, :] = bh
    b16[144:288, :] = bl
    for i in range(wide // 128):
        part = (iota((128, 128), 0) + 128 * i - 64) // BS
        inside = jnp.logical_and(part >= 0, part < cells)
        s2[128 * i : 128 * i + 128, :] = onehot(
            jnp.logical_and(inside, part == iota((128, 128), 1))
        ).astype(BF16)

    whole(ext.at[pl.ds(16, 16), own], edge_sem)
    pl.semaphore_wait(
        barrier,
        7 + 2 * crosses_up.astype(I32) + 2 * crosses_down.astype(I32),
    )

    for d in (1, 7):
        signal(ready.at[0], at(px, beside_y(d), col))
        signal(ready.at[0], at(beside_x(d), py, col))

    @pl.when(up)
    def _():
        send(ext.at[first8, own], ext.at[bottom, own], halo_send.at[1], halo_recv.at[1], (stripe, row - 1, col))
        send(ext.at[first8, inner], ext.at[bottom, pad_there], halo_send.at[1], halo_recv.at[1], (stripe, row - 1, other))

    @pl.when(down)
    def _():
        send(ext.at[last8, own], ext.at[top, own], halo_send.at[2], halo_recv.at[2], (stripe, row + 1, col))
        send(ext.at[last8, inner], ext.at[top, pad_there], halo_send.at[2], halo_recv.at[2], (stripe, row + 1, other))

    for i in range(8):
        if i % 2 == 0:
            start = spans[i][0]
            whole(ext.at[pl.ds(16 + start, spans[i + 1][1] - start), own], load_sem.at[i // 2])
        x = ext[16 + 32 * i : 48 + 32 * i, 128 : cols + 128].astype(F32)
        rs[8 * i : 8 * i + 8, :] = x.reshape(4, 8, cols).sum(axis=0)
        cb[16 + 32 * i : 48 + 32 * i, 128 : cols + 128] = x.astype(BF16)
    sums = dot_exact(rs[...], s1[...])
    means = sums.reshape(8, 8, 128).sum(axis=1) * (1.0 / (255.0 * BS * BS))
    mbuf[mine] = packed(means)

    send(ext.at[body, inner], ext.at[body, pad_there], halo_send.at[0], halo_recv.at[0], at(px, py, other))

    def spread_y(buf, sem, order, partner):
        for d in order:
            for c in (0, 1):
                send(buf.at[mine], buf.at[mine], sem.at[0], sem.at[1], at(px, beside_y(d), c))
        if partner:
            send(buf.at[mine], buf.at[mine], sem.at[0], sem.at[1], at(px, py, other))

    def collect_y(buf, sem):
        whole(buf.at[pl.ds(0, 2 * SIDE - 1)], sem.at[1])

    def spread_x(buf, sem):
        for d in ORDER:
            send(buf.at[px], buf.at[px], sem.at[0], sem.at[1], at(beside_x(d), py, col))

    def collect_x(buf, sem):
        whole(buf.at[pl.ds(0, SIDE - 1)], sem.at[1])

    def spread_slabs(buf, sem):
        @pl.when(px < SIDE - 1)
        def _():
            send(buf.at[pl.ds(64, 48), :], buf.at[pl.ds(0, 48), :],
                 sem.at[0], sem.at[2], at(px + 1, py, col))

        @pl.when(px > 0)
        def _():
            send(buf.at[pl.ds(48, 48), :], buf.at[pl.ds(112, 48), :],
                 sem.at[1], sem.at[3], at(px - 1, py, col))

    def collect_slabs(buf, sem):
        @pl.when(px > 0)
        def _():
            whole(buf.at[pl.ds(0, 48), :], sem.at[2])

        @pl.when(px < SIDE - 1)
        def _():
            whole(buf.at[pl.ds(112, 48), :], sem.at[3])

    def pieces(ref, parts, lanes):
        found = [ref[first : first + count, lanes] for first, count in parts]
        return found[0] if len(found) == 1 else jnp.concatenate(found, axis=0)

    def put(ref, parts, lanes, value):
        at_row = 0
        for first, count in parts:
            ref[first : first + count, lanes] = value[at_row : at_row + count]
            at_row += count

    def blur_across(src_hi, src_lo, dst_hi, dst_lo, parts, tiles):
        for j in range(tiles):
            window, lanes = slice(128 * j, 128 * j + 256), slice(128 * j, 128 * j + 128)
            wide_part = dot(pieces(src_hi, parts, window), wcat[...])
            part = wide_part[:, 0:128] + wide_part[:, 128:256]
            if src_lo is not None:
                part = part + dot(pieces(src_lo, parts, window), wcat[:, 0:128])
            high, low = split(part)
            put(dst_hi, parts, lanes, high)
            put(dst_lo, parts, lanes, low)

    def shift_coverage(parts):
        count = sum(n for _, n in parts)
        half = iota((count, 128), 1) < 64
        turned = pltpu.roll(pieces(ext, parts, slice(0, 128)).astype(F32), 64, 1)
        for j in range(wide // 128):
            following = pieces(ext, parts, slice(128 * j + 128, 128 * j + 256)).astype(F32)
            following = pltpu.roll(following, 64, 1)
            put(cs, parts, slice(128 * j, 128 * j + 128), jnp.where(half, turned, following))
            turned = following

    def blur_down(count, depth, high, low, first, lanes):
        both = jnp.concatenate([b16[0:count, 0:depth], b16[144 : 144 + count, 0:depth]], 0)
        here = slice(first, first + depth)
        result = dot(both, high[here, lanes])
        return result[0:count] + result[count:] + dot(b16[0:count, 0:depth], low[here, lanes])

    pl.semaphore_wait(ready.at[0], 4)
    for d in (2, 6):
        signal(ready.at[1], at(px, beside_y(d), col))
        signal(ready.at[1], at(beside_x(d), py, col))

    spread_y(mbuf, m_sem, (2, 6, 1, 7), True)
    body_rows, edge_rows = ((16, 256),), ((0, 16), (272, 16))
    whole(ext.at[body, pad_here], halo_recv.at[0])
    for pad in (0, cols + 128):
        cb[16:272, pad : pad + 128] = ext[16:272, pad : pad + 128].astype(F32).astype(BF16)
    blur_across(cb, None, hhi, hlo, body_rows, wide // 128)

    shift_coverage(body_rows)

    tiles = [slice(256 * j, 256 * j + 256) for j in range(wide // 256)]
    if wide % 256:
        tiles.append(slice(wide - 128, wide))

    def main_rows(lanes):
        width = lanes.stop - lanes.start
        for block in (0, 1):
            here = slice(32 + 112 * block, 144 + 112 * block)
            t = 1.5 - blur_down(112, 144, hhi, hlo, 16 + 112 * block, lanes) * (0.5 / 255.0)
            tt[here, lanes] = t
            product = cs[here, lanes] * t
            whole = product[16:112] if block == 0 else product[0:96]
            half = product[0:16] if block == 0 else product[96:112]
            whole = whole.reshape(3, 4, 8, width).sum(axis=1).reshape(24, width)
            asum[8 + 24 * block : 32 + 24 * block, lanes] = whole
            asum[56 * block : 56 * block + 8, lanes] = half[0:8] + half[8:16]

    for lanes in tiles:
        main_rows(lanes)

    pl.semaphore_wait(ready.at[1], 4)
    spread_y(mbuf, m_sem, (4, 3, 5), False)

    part, side = iota((128, 192), 0) // 64, lax.rem(iota((128, 192), 0) // 32, 2)
    piece = iota((128, 192), 1) // 48
    value = taps_of(lax.rem(iota((128, 192), 1), 48) - lax.rem(iota((128, 192), 0), 32) - 16 * side)
    high, low = split(value)
    value = jnp.where(part == 0, high.astype(F32), jnp.where(lax.rem(piece, 2) == 0, low.astype(F32), 0.0))
    edge_taps = jnp.where(side == piece // 2, value, 0.0).astype(BF16)


    @pl.when(up)
    def _():
        whole(ext.at[top, both], halo_recv.at[2])

    @pl.when(down)
    def _():
        whole(ext.at[bottom, both], halo_recv.at[1])

    for first in (0, 272):
        cb[first : first + 16, :] = ext[first : first + 16, :].astype(F32).astype(BF16)
    blur_across(cb, None, hhi, hlo, edge_rows, wide // 128)
    shift_coverage(edge_rows)
    for lanes in tiles:
        inputs = jnp.concatenate(
            [hhi[0:48, lanes], hlo[0:48, lanes], hhi[240:288, lanes], hlo[240:288, lanes]], 0
        )
        result = dot(edge_taps, inputs)
        t = 1.5 - (result[0:64] + result[64:128]) * (0.5 / 255.0)
        tt[0:32, lanes] = t[0:32]
        tt[256:288, lanes] = t[32:64]
        product = cs[16:32, lanes] * t[16:32]
        asum[64:72, lanes] = product[0:8] + product[8:16]
        product = cs[256:272, lanes] * t[32:48]
        asum[72:80, lanes] = product[0:8] + product[8:16]
    sums = dot_exact(asum[...], s2[...]).reshape(10, 8, 128).sum(axis=1)
    cell_row = iota((8, 128), 0)
    sums = (
        sums[0:8]
        + jnp.where(cell_row == 0, sums[8:9], 0.0)
        + jnp.where(cell_row == 7, sums[9:10], 0.0)
    )
    abuf[mine] = packed(sums * (1.0 / (255.0 * BS * BS)))
    spread_y(abuf, a_sem, ORDER, True)

    collect_y(mbuf, m_sem)
    mx = unpacked(mbuf)
    mext[48:112, :] = mx
    to_region = jnp.where(
        iota((128, 128), 0) // 8 == lax.rem(iota((128, 128), 1), 16), 1.0 / 64.0, 0.0
    ).astype(BF16)
    own_lanes = iota((64, 128), 1) // 16 == iota((64, 128), 0) // 8

    def region_row(field):
        return jnp.where(own_lanes, dot_exact(field, to_region), 0.0).sum(axis=0, keepdims=True)

    pbuf[px] = region_row(mx)
    spread_slabs(mext, ms_sem)
    spread_x(pbuf, p_sem)
    for i in range(wide // 128):
        cell = (iota((128, 128), 1) + 128 * i + cols * col - 64 + 128) // BS - 4
        sps[:, 128 * i : 128 * i + 128] = onehot(cell == iota((128, 128), 0)).astype(BF16)

    across = gauss_of(iota((128, 128), 0) - iota((128, 128), 1))
    across = jnp.where(
        jnp.logical_and(iota((128, 128), 0) < 2 * cells, iota((128, 128), 1) < 2 * cells), across, 0.0
    )
    ah, al = split(across)

    def dot_across(field):
        fh, fl = split(field)
        return dot(fh, ah) + (dot(fl, ah) + dot(fh, al))

    for copy in fog_loads:
        copy.wait()
    kr = fr[...]
    kr = kr / jnp.sum(kr, axis=1, keepdims=True)
    kc = fc[...]
    kc = kc / jnp.sum(kc, axis=1, keepdims=True)
    nreg = 2 * cells // 8
    pick = onehot(lax.rem(iota((128, nreg), 0), 16) == iota((128, nreg), 1))
    kct = kc.T
    to_cells = dot_exact(kct, onehot(iota((nreg, 128), 1) // 8 == iota((nreg, 128), 0)))
    to_lanes = dot_exact(kct, onehot(lax.rem(iota((nreg, 128), 1), 16) == iota((nreg, 128), 0)))
    zc = exact_dot(pick, to_cells)
    zl = exact_dot(pick, to_lanes)
    zboth = jnp.concatenate([zc, zl], axis=1)
    in_block = iota((64, 128), 1) // 16 == lax.rem(iota((64, 128), 0), 8)
    kr_24 = exact_dot(onehot(row - 1 + iota((24, 64), 0) // 8 == iota((24, 64), 1)), kr)
    kr_160 = exact_dot(onehot(8 * px - 6 + iota((160, 64), 0) // 8 == iota((160, 64), 1)), kr)
    own_kr = jnp.where(iota((64, 64), 0) == row, kr, 0.0).sum(axis=0, keepdims=True)
    own_kr = jnp.where(iota((8, 64), 1) // 8 == iota((8, 64), 0), own_kr, 0.0)
    own_kr = dot_exact(own_kr, onehot(lax.rem(iota((64, 128), 0), 8) == iota((64, 128), 1) // 16))
    zph, zpl = split(dot_exact(0.2 * zc, sps[:, 64 : cols + 64]))
    zp[0] = zph
    zp[1] = zpl

    collect_slabs(mext, ms_sem)
    swept = dot_across(mext[...])
    back_x = dot3(gauss_of(iota((64, 160), 0) - iota((64, 160), 1) + 48), swept)
    back_24 = dot3(gauss_of(iota((24, 160), 0) - iota((24, 160), 1) + 40 + 8 * py), swept)

    collect_y(abuf, a_sem)
    ax = unpacked(abuf)
    bx = ax - 0.3 * back_x * mext[48:112, :]
    bext[48:112, :] = bx
    ebuf[px] = region_row(bx)
    spread_x(ebuf, e_sem)
    spread_slabs(bext, bs_sem)

    collect_x(pbuf, p_sem)
    regions = pbuf[...]
    spread = jnp.broadcast_to(regions, (8, 8, 128)).reshape(64, 128)
    fog_wide = dot3(jnp.where(in_block, spread, 0.0), zboth)
    fog_24 = dot3(kr_24, fog_wide[:, 0:128])

    coarse = 0.3 * back_24 + 0.2 * fog_24
    row24[...] = dot_exact(coarse, sps[...])
    fog_lanes = jnp.where(in_block, dot3(kr, fog_wide[:, 128:256]), 0.0).reshape(8, 8, 128).sum(axis=1)
    fog_160 = dot3(kr_160, fog_wide[:, 0:128])
    for first, count, place in [(0, 16, 7)] + [(16 + 32 * i, 32, 8 + i) for i in range(8)] + [(272, 16, 16)]:
        here = slice(first, first + count)
        dose = tt[here, :] - row24[place : place + 1, :]
        tt[here, :] = dose
        high, low = split(cs[here, :] * dose)
        qhi[here, :] = high
        qlo[here, :] = low
    blur_across(qhi, qlo, h2hi, h2lo, ((0, 288),), cols // 128)
    left = iota((128, 128), 1) < 64
    for j in range(cols // 256):
        lanes = slice(256 * j, 256 * j + 256)
        for block in (0, 1):
            fine = blur_down(128, 160, h2hi, h2lo, 128 * block, lanes)
            here = slice(16 + 128 * block, 144 + 128 * block)
            turned = [pltpu.roll(tt[here, 256 * j + 128 * i : 256 * j + 128 * i + 128], 64, 1) for i in range(3)]
            for i in (0, 1):
                dose = jnp.where(left, turned[i], turned[i + 1])
                x_out[128 * block : 128 * block + 128, 256 * j + 128 * i : 256 * j + 128 * i + 128] = (
                    dose + 0.5 - fine[:, 128 * i : 128 * i + 128] * (0.5 / 255.0)
                )

    whole(mbuf.at[pl.ds(0, 2 * SIDE - 1)], m_sem.at[0])
    whole(abuf.at[pl.ds(0, 2 * SIDE - 1)], a_sem.at[0])
    whole(pbuf.at[pl.ds(0, SIDE - 1)], p_sem.at[0])
    whole(ebuf.at[pl.ds(0, SIDE - 1)], e_sem.at[0])
    whole(ext.at[body, pad_here], halo_send.at[0])

    @pl.when(up)
    def _():
        whole(ext.at[top, both], halo_send.at[1])

    @pl.when(down)
    def _():
        whole(ext.at[bottom, both], halo_send.at[2])

    @pl.when(px < SIDE - 1)
    def _():
        whole(mext.at[pl.ds(0, 48), :], ms_sem.at[0])
        whole(bext.at[pl.ds(0, 48), :], bs_sem.at[0])

    @pl.when(px > 0)
    def _():
        whole(mext.at[pl.ds(112, 48), :], ms_sem.at[1])
        whole(bext.at[pl.ds(112, 48), :], bs_sem.at[1])

    collect_slabs(bext, bs_sem)
    means2 = bext[...] - 0.2 * fog_160 * mext[...]
    back2 = dot3(gauss_of(iota((8, 160), 0) - iota((8, 160), 1) + 48 + 8 * py), dot_across(means2))
    coarse_out[...] = dot_exact(0.3 * back2, sps[:, 64 : cols + 64])
    fog_known = 0.2 * fog_lanes * regions.reshape(8, 128)
    collect_x(ebuf, e_sem)
    fog_mean2 = ebuf[...].reshape(8, 128) - fog_known
    weighted = jnp.broadcast_to((own_kr * fog_mean2).sum(axis=0, keepdims=True), (8, 128))
    high, low = split(weighted)
    fog2 = dot(high, zp[0]) + (dot(low, zp[0]) + dot(high, zp[1]))
    coarse_out[...] = coarse_out[...] + fog2


def finish_kernel(x, coarse, out, buf, sem):
    cols = coarse.shape[1]
    copies = []
    for i in range(8):
        here = pl.ds(32 * i, 32)
        buf[32 * i : 32 * i + 32, :] = x[32 * i : 32 * i + 32, :] - coarse[i : i + 1, :]
        copy = pltpu.make_async_copy(buf.at[here, :], out.at[here, :], sem.at[i])
        copy.start()
        copies.append(copy)
    for copy in copies:
        copy.wait()


def shards(coverage, fog_rows, fog_cols):
    rows, cols = coverage.shape
    wide = cols + 128
    dma = pltpu.SemaphoreType.DMA
    hbm = pl.BlockSpec(memory_space=pl.ANY)
    vmem = pl.BlockSpec(memory_space=pltpu.VMEM)
    x, coarse = pl.pallas_call(
        correct_kernel,
        out_shape=(
            jax.ShapeDtypeStruct((rows, cols), F32),
            jax.ShapeDtypeStruct((8, cols), F32),
        ),
        in_specs=[pl.BlockSpec(memory_space=pltpu.MemorySpace.HBM)] * 3,
        out_specs=(vmem, vmem),
        scratch_shapes=[
            pltpu.VMEM((288, cols + 256), I32),
            pltpu.VMEM((288, cols + 256), BF16),
            pltpu.VMEM((64, cols), F32),
            pltpu.VMEM((288, wide), F32),
            pltpu.VMEM((288, wide), BF16),
            pltpu.VMEM((288, wide), BF16),
            pltpu.VMEM((288, wide), F32),
            pltpu.VMEM((80, wide), F32),
            pltpu.VMEM((288, wide), BF16),
            pltpu.VMEM((288, wide), BF16),
            pltpu.VMEM((288, cols), BF16),
            pltpu.VMEM((288, cols), BF16),
            pltpu.VMEM((cols, 128), BF16),
            pltpu.VMEM((wide, 128), BF16),
            pltpu.VMEM((128, wide), BF16),
            pltpu.VMEM((256, 256), BF16),
            pltpu.VMEM((288, 160), BF16),
            pltpu.VMEM((2, 128, cols), BF16),
            pltpu.VMEM((24, wide), F32),
            pltpu.VMEM((2 * SIDE, 4, 128), F32),
            pltpu.VMEM((160, 128), F32),
            pltpu.VMEM((SIDE, 1, 128), F32),
            pltpu.VMEM((2 * SIDE, 4, 128), F32),
            pltpu.VMEM((160, 128), F32),
            pltpu.VMEM((SIDE, 1, 128), F32),
            pltpu.VMEM(fog_rows.shape, F32),
            pltpu.VMEM(fog_cols.shape, F32),
            dma(()), dma((4,)), dma((2,)), dma((3,)), dma((3,)), pltpu.SemaphoreType.REGULAR((2,)),
            dma((2,)), dma((2,)), dma((2,)), dma((2,)), dma((4,)), dma((4,)),
        ],
        compiler_params=pltpu.CompilerParams(
            collective_id=0, has_side_effects=True, vmem_limit_bytes=44 * 1024 * 1024
        ),
    )(*[pltpu.with_memory_space_constraint(v, pltpu.MemorySpace.HBM) for v in (coverage, fog_rows, fog_cols)])
    return pl.pallas_call(
        finish_kernel,
        out_shape=jax.ShapeDtypeStruct((rows, cols), F32),
        in_specs=[vmem, vmem],
        out_specs=hbm,
        scratch_shapes=[pltpu.VMEM((rows, cols), F32), dma((8,))],
        compiler_params=pltpu.CompilerParams(vmem_limit_bytes=8 * 1024 * 1024),
    )(x, coarse)


def solution(mesh):
    placed = (P(("stripe", "row"), "col"), P(), P())
    return jax.shard_map(
        shards, mesh=mesh, in_specs=placed, out_specs=P(("stripe", "row"), "col"), check_vma=False
    )
```

```python
import math

import jax
import jax.numpy as jnp
from jax import lax
from jax.experimental import pallas as pl
from jax.experimental.pallas import tpu as pltpu
from jax.sharding import PartitionSpec as P

BS = 32
FB = 256
HALO = 4
BSIG = 16
REACH = 40
SIDE = 8
MESH = pl.DeviceIdType.MESH
F32 = jnp.float32
BF16 = jnp.bfloat16
I32 = jnp.int32
ORDER = (4, 3, 5, 2, 6, 1, 7)

TAPS = [math.exp(-(k * k) / (2 * 1.25**2)) for k in range(-HALO, HALO + 1)]
TAP_SCALE = 1.0 / sum(TAPS)
GAUSS_SCALE = 1.0 / (BSIG * math.sqrt(2.0 * math.pi))


def iota(shape, dim):
    return lax.broadcasted_iota(I32, shape, dim)


def onehot(condition):
    return jnp.where(condition, 1.0, 0.0).astype(F32)


def taps_of(offset):
    square = (offset * offset).astype(F32)
    value = jnp.exp(square * (-1.0 / (2 * 1.25**2))) * TAP_SCALE
    return jnp.where(jnp.abs(offset) <= HALO, value, 0.0)


def gauss_of(offset):
    square = (offset * offset).astype(F32)
    value = jnp.exp(square * (-0.5 / (BSIG * BSIG))) * GAUSS_SCALE
    return jnp.where(jnp.abs(offset) <= REACH, value, 0.0)


def split(value):
    high = value.astype(BF16)
    return high, (value - high.astype(F32)).astype(BF16)


def dot(a, b):
    return jnp.dot(a, b, preferred_element_type=F32)


def dot_exact(a, b):
    high, low = split(a)
    b = b.astype(BF16)
    return dot(high, b) + dot(low, b)


def exact_dot(a, b):
    high, low = split(b)
    a = a.astype(BF16)
    return dot(a, high) + dot(a, low)


def dot3(a, b):
    ah, al = split(a)
    bh, bl = split(b)
    return dot(ah, bh) + (dot(al, bh) + dot(ah, bl))


def packed(tile):
    return tile[0:4] + pltpu.roll(tile, 64, 1)[4:8]


def unpacked(buf):
    left = iota((4, 128), 1) < 64
    parts = []
    for y in range(SIDE):
        first, second = buf[y], buf[SIDE + y]
        parts.append(jnp.where(left, first, pltpu.roll(second, 64, 1)))
        parts.append(jnp.where(left, pltpu.roll(first, 64, 1), second))
    return jnp.concatenate(parts, axis=0)


def correct_kernel(
    cov, fogr, fogc, x_out, coarse_out,
    ext, cb, rs, cs, hhi, hlo, tt, asum, qhi, qlo, h2hi, h2lo,
    s1, s2, sps, wcat, b16, zp, row24, mbuf, mext, pbuf, abuf, bext, ebuf, fr, fc,
    edge_sem, load_sem, fog_sem, halo_send, halo_recv, ready,
    m_sem, a_sem, p_sem, e_sem, ms_sem, bs_sem,
):
    stripe = lax.axis_index("stripe")
    row = lax.axis_index("row")
    col = lax.axis_index("col")
    px = row // SIDE
    py = lax.rem(row, SIDE)
    other = 1 - col
    rows, cols = 256, cov.shape[1]
    cells = cols // BS
    wide = cols + 128
    last = SIDE * SIDE - 1
    mine = col * SIDE + py

    own = pl.ds(128, cols)
    first8, last8 = pl.ds(16, 8), pl.ds(264, 8)
    for at_row in (0, 248):
        pltpu.make_async_copy(
            cov.at[pl.ds(at_row, 8), :], ext.at[pl.ds(16 + at_row, 8), own], edge_sem
        ).start()
    spans = [(8, 32), (32, 64), (64, 96), (96, 128), (128, 160), (160, 192), (192, 224), (224, 248)]
    for i, (start, stop) in enumerate(spans):
        pltpu.make_async_copy(
            cov.at[pl.ds(start, stop - start), :],
            ext.at[pl.ds(16 + start, stop - start), own],
            load_sem.at[i // 2],
        ).start()
    fog_loads = [
        pltpu.make_async_copy(fogr, fr, fog_sem.at[0]),
        pltpu.make_async_copy(fogc, fc, fog_sem.at[1]),
    ]
    for copy in fog_loads:
        copy.start()

    def whole(ref, sem):
        pltpu.make_async_copy(ref, ref, sem).wait()

    ext[0:16, :] = jnp.zeros((16, cols + 256), I32)
    ext[272:288, :] = jnp.zeros((16, cols + 256), I32)
    ext[16:272, 0:128] = jnp.zeros((256, 128), I32)
    ext[16:272, cols + 128 : cols + 256] = jnp.zeros((256, 128), I32)
    for buf in (mext, bext):
        buf[0:48, :] = jnp.zeros((48, 128), F32)
        buf[112:160, :] = jnp.zeros((48, 128), F32)

    def at(x, y, c):
        return (stripe, x * SIDE + y, c)

    def beside_y(d):
        return lax.rem(py + d, SIDE)

    def beside_x(d):
        return lax.rem(px + d, SIDE)

    barrier = pltpu.get_barrier_semaphore()

    def signal(sem, target):
        pl.semaphore_signal(sem, inc=1, device_id=target, device_id_type=MESH)

    crosses_up = jnp.logical_and(py == 0, px > 0)
    crosses_down = jnp.logical_and(py == SIDE - 1, px < SIDE - 1)
    for d in (1, 7):
        for c in (0, 1):
            signal(barrier, at(px, beside_y(d), c))
        signal(barrier, at(beside_x(d), py, col))
    signal(barrier, at(px, py, other))

    @pl.when(crosses_up)
    def _():
        for c in (0, 1):
            signal(barrier, (stripe, row - 1, c))

    @pl.when(crosses_down)
    def _():
        for c in (0, 1):
            signal(barrier, (stripe, row + 1, c))

    def send(src, dst, s_sem, r_sem, target):
        pltpu.make_async_remote_copy(
            src_ref=src, dst_ref=dst, send_sem=s_sem, recv_sem=r_sem,
            device_id=target, device_id_type=MESH,
        ).start()

    inner = pl.ds(pl.multiple_of((1 - col) * (cols - 128) + 128, 128), 128)
    pad_there = pl.ds(pl.multiple_of(col * (cols + 128), 128), 128)
    pad_here = pl.ds(pl.multiple_of(other * (cols + 128), 128), 128)
    body, top, bottom = pl.ds(16, 256), pl.ds(8, 8), pl.ds(272, 8)
    both = pl.ds(0, cols + 128)
    up, down = row > 0, row < last

    for i in range(cols // 256):
        part = (iota((256, 128), 0) + 256 * i) // BS
        s1[256 * i : 256 * i + 256, :] = onehot(part == iota((256, 128), 1)).astype(BF16)
    wh, wl = split(taps_of(iota((256, 128), 0) - iota((256, 128), 1) - 64))
    wcat[:, 0:128] = wh
    wcat[:, 128:256] = wl
    bh, bl = split(taps_of(iota((144, 160), 1) - iota((144, 160), 0) - 16))
    b16[0:144, :] = bh
    b16[144:288, :] = bl
    for i in range(wide // 128):
        part = (iota((128, 128), 0) + 128 * i - 64) // BS
        inside = jnp.logical_and(part >= 0, part < cells)
        s2[128 * i : 128 * i + 128, :] = onehot(
            jnp.logical_and(inside, part == iota((128, 128), 1))
        ).astype(BF16)

    whole(ext.at[pl.ds(16, 16), own], edge_sem)
    pl.semaphore_wait(
        barrier,
        7 + 2 * crosses_up.astype(I32) + 2 * crosses_down.astype(I32),
    )

    for d in (1, 7):
        signal(ready.at[0], at(px, beside_y(d), col))
        signal(ready.at[0], at(beside_x(d), py, col))

    @pl.when(up)
    def _():
        send(ext.at[first8, own], ext.at[bottom, own], halo_send.at[1], halo_recv.at[1], (stripe, row - 1, col))
        send(ext.at[first8, inner], ext.at[bottom, pad_there], halo_send.at[1], halo_recv.at[1], (stripe, row - 1, other))

    @pl.when(down)
    def _():
        send(ext.at[last8, own], ext.at[top, own], halo_send.at[2], halo_recv.at[2], (stripe, row + 1, col))
        send(ext.at[last8, inner], ext.at[top, pad_there], halo_send.at[2], halo_recv.at[2], (stripe, row + 1, other))

    for i in range(8):
        if i % 2 == 0:
            start = spans[i][0]
            whole(ext.at[pl.ds(16 + start, spans[i + 1][1] - start), own], load_sem.at[i // 2])
        x = ext[16 + 32 * i : 48 + 32 * i, 128 : cols + 128].astype(F32)
        rs[8 * i : 8 * i + 8, :] = x.reshape(4, 8, cols).sum(axis=0)
        cb[16 + 32 * i : 48 + 32 * i, 128 : cols + 128] = x.astype(BF16)
    sums = dot_exact(rs[...], s1[...])
    means = sums.reshape(8, 8, 128).sum(axis=1) * (1.0 / (255.0 * BS * BS))
    mbuf[mine] = packed(means)

    send(ext.at[body, inner], ext.at[body, pad_there], halo_send.at[0], halo_recv.at[0], at(px, py, other))

    def spread_y(buf, sem, order, partner):
        for d in order:
            for c in (0, 1):
                send(buf.at[mine], buf.at[mine], sem.at[0], sem.at[1], at(px, beside_y(d), c))
        if partner:
            send(buf.at[mine], buf.at[mine], sem.at[0], sem.at[1], at(px, py, other))

    def collect_y(buf, sem):
        whole(buf.at[pl.ds(0, 2 * SIDE - 1)], sem.at[1])

    def spread_x(buf, sem):
        for d in ORDER:
            send(buf.at[px], buf.at[px], sem.at[0], sem.at[1], at(beside_x(d), py, col))

    def collect_x(buf, sem):
        whole(buf.at[pl.ds(0, SIDE - 1)], sem.at[1])

    def spread_slabs(buf, sem):
        @pl.when(px < SIDE - 1)
        def _():
            send(buf.at[pl.ds(64, 48), :], buf.at[pl.ds(0, 48), :],
                 sem.at[0], sem.at[2], at(px + 1, py, col))

        @pl.when(px > 0)
        def _():
            send(buf.at[pl.ds(48, 48), :], buf.at[pl.ds(112, 48), :],
                 sem.at[1], sem.at[3], at(px - 1, py, col))

    def collect_slabs(buf, sem):
        @pl.when(px > 0)
        def _():
            whole(buf.at[pl.ds(0, 48), :], sem.at[2])

        @pl.when(px < SIDE - 1)
        def _():
            whole(buf.at[pl.ds(112, 48), :], sem.at[3])

    def pieces(ref, parts, lanes):
        found = [ref[first : first + count, lanes] for first, count in parts]
        return found[0] if len(found) == 1 else jnp.concatenate(found, axis=0)

    def put(ref, parts, lanes, value):
        at_row = 0
        for first, count in parts:
            ref[first : first + count, lanes] = value[at_row : at_row + count]
            at_row += count

    def blur_across(src_hi, src_lo, dst_hi, dst_lo, parts, tiles):
        for j in range(tiles):
            window, lanes = slice(128 * j, 128 * j + 256), slice(128 * j, 128 * j + 128)
            wide_part = dot(pieces(src_hi, parts, window), wcat[...])
            part = wide_part[:, 0:128] + wide_part[:, 128:256]
            if src_lo is not None:
                part = part + dot(pieces(src_lo, parts, window), wcat[:, 0:128])
            high, low = split(part)
            put(dst_hi, parts, lanes, high)
            put(dst_lo, parts, lanes, low)

    def shift_coverage(parts):
        count = sum(n for _, n in parts)
        half = iota((count, 128), 1) < 64
        turned = pltpu.roll(pieces(ext, parts, slice(0, 128)).astype(F32), 64, 1)
        for j in range(wide // 128):
            following = pieces(ext, parts, slice(128 * j + 128, 128 * j + 256)).astype(F32)
            following = pltpu.roll(following, 64, 1)
            put(cs, parts, slice(128 * j, 128 * j + 128), jnp.where(half, turned, following))
            turned = following

    def blur_down(count, depth, high, low, first, lanes):
        both = jnp.concatenate([b16[0:count, 0:depth], b16[144 : 144 + count, 0:depth]], 0)
        here = slice(first, first + depth)
        result = dot(both, high[here, lanes])
        return result[0:count] + result[count:] + dot(b16[0:count, 0:depth], low[here, lanes])

    pl.semaphore_wait(ready.at[0], 4)
    for d in (2, 6):
        signal(ready.at[1], at(px, beside_y(d), col))
        signal(ready.at[1], at(beside_x(d), py, col))

    spread_y(mbuf, m_sem, (2, 6, 1, 7), True)
    body_rows, edge_rows = ((16, 256),), ((0, 16), (272, 16))
    whole(ext.at[body, pad_here], halo_recv.at[0])
    for pad in (0, cols + 128):
        cb[16:272, pad : pad + 128] = ext[16:272, pad : pad + 128].astype(F32).astype(BF16)
    blur_across(cb, None, hhi, hlo, body_rows, wide // 128)

    shift_coverage(body_rows)

    tiles = [slice(256 * j, 256 * j + 256) for j in range(wide // 256)]
    if wide % 256:
        tiles.append(slice(wide - 128, wide))

    def main_rows(lanes):
        width = lanes.stop - lanes.start
        for block in (0, 1):
            here = slice(32 + 112 * block, 144 + 112 * block)
            t = 1.5 - blur_down(112, 144, hhi, hlo, 16 + 112 * block, lanes) * (0.5 / 255.0)
            tt[here, lanes] = t
            product = cs[here, lanes] * t
            whole = product[16:112] if block == 0 else product[0:96]
            half = product[0:16] if block == 0 else product[96:112]
            whole = whole.reshape(3, 4, 8, width).sum(axis=1).reshape(24, width)
            asum[8 + 24 * block : 32 + 24 * block, lanes] = whole
            asum[56 * block : 56 * block + 8, lanes] = half[0:8] + half[8:16]

    for lanes in tiles:
        main_rows(lanes)

    pl.semaphore_wait(ready.at[1], 4)
    spread_y(mbuf, m_sem, (4, 3, 5), False)

    part, side = iota((128, 192), 0) // 64, lax.rem(iota((128, 192), 0) // 32, 2)
    piece = iota((128, 192), 1) // 48
    value = taps_of(lax.rem(iota((128, 192), 1), 48) - lax.rem(iota((128, 192), 0), 32) - 16 * side)
    high, low = split(value)
    value = jnp.where(part == 0, high.astype(F32), jnp.where(lax.rem(piece, 2) == 0, low.astype(F32), 0.0))
    edge_taps = jnp.where(side == piece // 2, value, 0.0).astype(BF16)


    @pl.when(up)
    def _():
        whole(ext.at[top, both], halo_recv.at[2])

    @pl.when(down)
    def _():
        whole(ext.at[bottom, both], halo_recv.at[1])

    for first in (0, 272):
        cb[first : first + 16, :] = ext[first : first + 16, :].astype(F32).astype(BF16)
    blur_across(cb, None, hhi, hlo, edge_rows, wide // 128)
    shift_coverage(edge_rows)
    for lanes in tiles:
        inputs = jnp.concatenate(
            [hhi[0:48, lanes], hlo[0:48, lanes], hhi[240:288, lanes], hlo[240:288, lanes]], 0
        )
        result = dot(edge_taps, inputs)
        t = 1.5 - (result[0:64] + result[64:128]) * (0.5 / 255.0)
        tt[0:32, lanes] = t[0:32]
        tt[256:288, lanes] = t[32:64]
        product = cs[16:32, lanes] * t[16:32]
        asum[64:72, lanes] = product[0:8] + product[8:16]
        product = cs[256:272, lanes] * t[32:48]
        asum[72:80, lanes] = product[0:8] + product[8:16]
    sums = dot_exact(asum[...], s2[...]).reshape(10, 8, 128).sum(axis=1)
    cell_row = iota((8, 128), 0)
    sums = (
        sums[0:8]
        + jnp.where(cell_row == 0, sums[8:9], 0.0)
        + jnp.where(cell_row == 7, sums[9:10], 0.0)
    )
    abuf[mine] = packed(sums * (1.0 / (255.0 * BS * BS)))
    spread_y(abuf, a_sem, ORDER, True)

    collect_y(mbuf, m_sem)
    mx = unpacked(mbuf)
    mext[48:112, :] = mx
    to_region = jnp.where(
        iota((128, 128), 0) // 8 == lax.rem(iota((128, 128), 1), 16), 1.0 / 64.0, 0.0
    ).astype(BF16)
    own_lanes = iota((64, 128), 1) // 16 == iota((64, 128), 0) // 8

    def region_row(field):
        return jnp.where(own_lanes, dot_exact(field, to_region), 0.0).sum(axis=0, keepdims=True)

    pbuf[px] = region_row(mx)
    spread_slabs(mext, ms_sem)
    spread_x(pbuf, p_sem)
    for i in range(wide // 128):
        cell = (iota((128, 128), 1) + 128 * i + cols * col - 64 + 128) // BS - 4
        sps[:, 128 * i : 128 * i + 128] = onehot(cell == iota((128, 128), 0)).astype(BF16)

    across = gauss_of(iota((128, 128), 0) - iota((128, 128), 1))
    across = jnp.where(
        jnp.logical_and(iota((128, 128), 0) < 2 * cells, iota((128, 128), 1) < 2 * cells), across, 0.0
    )
    ah, al = split(across)

    def dot_across(field):
        fh, fl = split(field)
        return dot(fh, ah) + (dot(fl, ah) + dot(fh, al))

    for copy in fog_loads:
        copy.wait()
    kr = fr[...]
    kr = kr / jnp.sum(kr, axis=1, keepdims=True)
    kc = fc[...]
    kc = kc / jnp.sum(kc, axis=1, keepdims=True)
    nreg = 2 * cells // 8
    pick = onehot(lax.rem(iota((128, nreg), 0), 16) == iota((128, nreg), 1))
    kct = kc.T
    to_cells = dot_exact(kct, onehot(iota((nreg, 128), 1) // 8 == iota((nreg, 128), 0)))
    to_lanes = dot_exact(kct, onehot(lax.rem(iota((nreg, 128), 1), 16) == iota((nreg, 128), 0)))
    zc = exact_dot(pick, to_cells)
    zl = exact_dot(pick, to_lanes)
    zboth = jnp.concatenate([zc, zl], axis=1)
    in_block = iota((64, 128), 1) // 16 == lax.rem(iota((64, 128), 0), 8)
    kr_24 = exact_dot(onehot(row - 1 + iota((24, 64), 0) // 8 == iota((24, 64), 1)), kr)
    kr_160 = exact_dot(onehot(8 * px - 6 + iota((160, 64), 0) // 8 == iota((160, 64), 1)), kr)
    own_kr = jnp.where(iota((64, 64), 0) == row, kr, 0.0).sum(axis=0, keepdims=True)
    own_kr = jnp.where(iota((8, 64), 1) // 8 == iota((8, 64), 0), own_kr, 0.0)
    own_kr = dot_exact(own_kr, onehot(lax.rem(iota((64, 128), 0), 8) == iota((64, 128), 1) // 16))
    zph, zpl = split(dot_exact(0.2 * zc, sps[:, 64 : cols + 64]))
    zp[0] = zph
    zp[1] = zpl

    collect_slabs(mext, ms_sem)
    swept = dot_across(mext[...])
    back_x = dot3(gauss_of(iota((64, 160), 0) - iota((64, 160), 1) + 48), swept)
    back_24 = dot3(gauss_of(iota((24, 160), 0) - iota((24, 160), 1) + 40 + 8 * py), swept)

    collect_y(abuf, a_sem)
    ax = unpacked(abuf)
    bx = ax - 0.3 * back_x * mext[48:112, :]
    bext[48:112, :] = bx
    ebuf[px] = region_row(bx)
    spread_x(ebuf, e_sem)
    spread_slabs(bext, bs_sem)

    collect_x(pbuf, p_sem)
    regions = pbuf[...]
    spread = jnp.broadcast_to(regions, (8, 8, 128)).reshape(64, 128)
    fog_wide = dot3(jnp.where(in_block, spread, 0.0), zboth)
    fog_24 = dot3(kr_24, fog_wide[:, 0:128])

    coarse = 0.3 * back_24 + 0.2 * fog_24
    row24[...] = dot_exact(coarse, sps[...])
    fog_lanes = jnp.where(in_block, dot3(kr, fog_wide[:, 128:256]), 0.0).reshape(8, 8, 128).sum(axis=1)
    fog_160 = dot3(kr_160, fog_wide[:, 0:128])
    for first, count, place in [(0, 16, 7)] + [(16 + 32 * i, 32, 8 + i) for i in range(8)] + [(272, 16, 16)]:
        here = slice(first, first + count)
        high, low = split(cs[here, :] * (tt[here, :] - row24[place : place + 1, :]))
        qhi[here, :] = high
        qlo[here, :] = low
    blur_across(qhi, qlo, h2hi, h2lo, ((0, 288),), cols // 128)
    left = iota((128, 128), 1) < 64
    for j in range(cols // 256):
        lanes = slice(256 * j, 256 * j + 256)
        for block in (0, 1):
            fine = blur_down(128, 160, h2hi, h2lo, 128 * block, lanes)
            here = slice(16 + 128 * block, 144 + 128 * block)
            turned = [pltpu.roll(tt[here, 256 * j + 128 * i : 256 * j + 128 * i + 128], 64, 1) for i in range(3)]
            for i in (0, 1):
                dose = jnp.where(left, turned[i], turned[i + 1])
                x_out[128 * block : 128 * block + 128, 256 * j + 128 * i : 256 * j + 128 * i + 128] = (
                    dose + 0.5 - fine[:, 128 * i : 128 * i + 128] * (0.5 / 255.0)
                )

    whole(mbuf.at[pl.ds(0, 2 * SIDE - 1)], m_sem.at[0])
    whole(abuf.at[pl.ds(0, 2 * SIDE - 1)], a_sem.at[0])
    whole(pbuf.at[pl.ds(0, SIDE - 1)], p_sem.at[0])
    whole(ebuf.at[pl.ds(0, SIDE - 1)], e_sem.at[0])
    whole(ext.at[body, pad_here], halo_send.at[0])

    @pl.when(up)
    def _():
        whole(ext.at[top, both], halo_send.at[1])

    @pl.when(down)
    def _():
        whole(ext.at[bottom, both], halo_send.at[2])

    @pl.when(px < SIDE - 1)
    def _():
        whole(mext.at[pl.ds(0, 48), :], ms_sem.at[0])
        whole(bext.at[pl.ds(0, 48), :], bs_sem.at[0])

    @pl.when(px > 0)
    def _():
        whole(mext.at[pl.ds(112, 48), :], ms_sem.at[1])
        whole(bext.at[pl.ds(112, 48), :], bs_sem.at[1])

    collect_slabs(bext, bs_sem)
    means2 = bext[...] - 0.2 * fog_160 * mext[...]
    back2 = dot3(gauss_of(iota((8, 160), 0) - iota((8, 160), 1) + 48 + 8 * py), dot_across(means2))
    coarse_out[...] = dot_exact(0.3 * back2 + coarse[8:16], sps[:, 64 : cols + 64])
    fog_known = 0.2 * fog_lanes * regions.reshape(8, 128)
    collect_x(ebuf, e_sem)
    fog_mean2 = ebuf[...].reshape(8, 128) - fog_known
    weighted = jnp.broadcast_to((own_kr * fog_mean2).sum(axis=0, keepdims=True), (8, 128))
    high, low = split(weighted)
    fog2 = dot(high, zp[0]) + (dot(low, zp[0]) + dot(high, zp[1]))
    coarse_out[...] = coarse_out[...] + fog2


def finish_kernel(x, coarse, out, buf, sem):
    cols = coarse.shape[1]
    copies = []
    for i in range(8):
        here = pl.ds(32 * i, 32)
        buf[32 * i : 32 * i + 32, :] = x[32 * i : 32 * i + 32, :] - coarse[i : i + 1, :]
        copy = pltpu.make_async_copy(buf.at[here, :], out.at[here, :], sem.at[i])
        copy.start()
        copies.append(copy)
    for copy in copies:
        copy.wait()


def shards(coverage, fog_rows, fog_cols):
    rows, cols = coverage.shape
    wide = cols + 128
    dma = pltpu.SemaphoreType.DMA
    hbm = pl.BlockSpec(memory_space=pl.ANY)
    vmem = pl.BlockSpec(memory_space=pltpu.VMEM)
    x, coarse = pl.pallas_call(
        correct_kernel,
        out_shape=(
            jax.ShapeDtypeStruct((rows, cols), F32),
            jax.ShapeDtypeStruct((8, cols), F32),
        ),
        in_specs=[pl.BlockSpec(memory_space=pltpu.MemorySpace.HBM)] * 3,
        out_specs=(vmem, vmem),
        scratch_shapes=[
            pltpu.VMEM((288, cols + 256), I32),
            pltpu.VMEM((288, cols + 256), BF16),
            pltpu.VMEM((64, cols), F32),
            pltpu.VMEM((288, wide), F32),
            pltpu.VMEM((288, wide), BF16),
            pltpu.VMEM((288, wide), BF16),
            pltpu.VMEM((288, wide), F32),
            pltpu.VMEM((80, wide), F32),
            pltpu.VMEM((288, wide), BF16),
            pltpu.VMEM((288, wide), BF16),
            pltpu.VMEM((288, cols), BF16),
            pltpu.VMEM((288, cols), BF16),
            pltpu.VMEM((cols, 128), BF16),
            pltpu.VMEM((wide, 128), BF16),
            pltpu.VMEM((128, wide), BF16),
            pltpu.VMEM((256, 256), BF16),
            pltpu.VMEM((288, 160), BF16),
            pltpu.VMEM((2, 128, cols), BF16),
            pltpu.VMEM((24, wide), F32),
            pltpu.VMEM((2 * SIDE, 4, 128), F32),
            pltpu.VMEM((160, 128), F32),
            pltpu.VMEM((SIDE, 1, 128), F32),
            pltpu.VMEM((2 * SIDE, 4, 128), F32),
            pltpu.VMEM((160, 128), F32),
            pltpu.VMEM((SIDE, 1, 128), F32),
            pltpu.VMEM(fog_rows.shape, F32),
            pltpu.VMEM(fog_cols.shape, F32),
            dma(()), dma((4,)), dma((2,)), dma((3,)), dma((3,)), pltpu.SemaphoreType.REGULAR((2,)),
            dma((2,)), dma((2,)), dma((2,)), dma((2,)), dma((4,)), dma((4,)),
        ],
        compiler_params=pltpu.CompilerParams(
            collective_id=0, has_side_effects=True, vmem_limit_bytes=44 * 1024 * 1024
        ),
    )(*[pltpu.with_memory_space_constraint(v, pltpu.MemorySpace.HBM) for v in (coverage, fog_rows, fog_cols)])
    return pl.pallas_call(
        finish_kernel,
        out_shape=jax.ShapeDtypeStruct((rows, cols), F32),
        in_specs=[vmem, vmem],
        out_specs=hbm,
        scratch_shapes=[pltpu.VMEM((rows, cols), F32), dma((8,))],
        compiler_params=pltpu.CompilerParams(vmem_limit_bytes=8 * 1024 * 1024),
    )(x, coarse)


def solution(mesh):
    placed = (P(("stripe", "row"), "col"), P(), P())
    return jax.shard_map(
        shards, mesh=mesh, in_specs=placed, out_specs=P(("stripe", "row"), "col"), check_vma=False
    )
```

```python
import math

import jax
import jax.numpy as jnp
from jax import lax
from jax.experimental import pallas as pl
from jax.experimental.pallas import tpu as pltpu
from jax.sharding import PartitionSpec as P

BS = 32
FB = 256
HALO = 4
BSIG = 16
REACH = 40
SIDE = 8
MESH = pl.DeviceIdType.MESH
F32 = jnp.float32
BF16 = jnp.bfloat16
I32 = jnp.int32
ORDER = (4, 3, 5, 2, 6, 1, 7)

TAPS = [math.exp(-(k * k) / (2 * 1.25**2)) for k in range(-HALO, HALO + 1)]
TAP_SCALE = 1.0 / sum(TAPS)
GAUSS_SCALE = 1.0 / (BSIG * math.sqrt(2.0 * math.pi))


def iota(shape, dim):
    return lax.broadcasted_iota(I32, shape, dim)


def onehot(condition):
    return jnp.where(condition, 1.0, 0.0).astype(F32)


def taps_of(offset):
    square = (offset * offset).astype(F32)
    value = jnp.exp(square * (-1.0 / (2 * 1.25**2))) * TAP_SCALE
    return jnp.where(jnp.abs(offset) <= HALO, value, 0.0)


def gauss_of(offset):
    square = (offset * offset).astype(F32)
    value = jnp.exp(square * (-0.5 / (BSIG * BSIG))) * GAUSS_SCALE
    return jnp.where(jnp.abs(offset) <= REACH, value, 0.0)


def split(value):
    high = value.astype(BF16)
    return high, (value - high.astype(F32)).astype(BF16)


def dot(a, b):
    return jnp.dot(a, b, preferred_element_type=F32)


def dot_exact(a, b):
    high, low = split(a)
    b = b.astype(BF16)
    return dot(high, b) + dot(low, b)


def exact_dot(a, b):
    high, low = split(b)
    a = a.astype(BF16)
    return dot(a, high) + dot(a, low)


def dot3(a, b):
    ah, al = split(a)
    bh, bl = split(b)
    return dot(ah, bh) + (dot(al, bh) + dot(ah, bl))


def packed(tile):
    return tile[0:4] + pltpu.roll(tile, 64, 1)[4:8]


def unpacked(buf):
    left = iota((4, 128), 1) < 64
    parts = []
    for y in range(SIDE):
        first, second = buf[y], buf[SIDE + y]
        parts.append(jnp.where(left, first, pltpu.roll(second, 64, 1)))
        parts.append(jnp.where(left, pltpu.roll(first, 64, 1), second))
    return jnp.concatenate(parts, axis=0)


def correct_kernel(
    cov, fogr, fogc, x_out, coarse_out,
    ext, cb, rs, cs, hhi, hlo, tt, asum, qhi, qlo, h2hi, h2lo,
    s1, s2, sps, wcat, b16, zp, row24, mbuf, mext, pbuf, abuf, bext, ebuf, fr, fc,
    edge_sem, load_sem, fog_sem, halo_send, halo_recv, ready,
    m_sem, a_sem, p_sem, e_sem, ms_sem, bs_sem,
):
    stripe = lax.axis_index("stripe")
    row = lax.axis_index("row")
    col = lax.axis_index("col")
    px = row // SIDE
    py = lax.rem(row, SIDE)
    other = 1 - col
    rows, cols = 256, cov.shape[1]
    cells = cols // BS
    wide = cols + 128
    last = SIDE * SIDE - 1
    mine = col * SIDE + py

    own = pl.ds(128, cols)
    first8, last8 = pl.ds(16, 8), pl.ds(264, 8)
    for at_row in (0, 248):
        pltpu.make_async_copy(
            cov.at[pl.ds(at_row, 8), :], ext.at[pl.ds(16 + at_row, 8), own], edge_sem
        ).start()
    spans = [(8, 32), (32, 64), (64, 96), (96, 128), (128, 160), (160, 192), (192, 224), (224, 248)]
    for i, (start, stop) in enumerate(spans):
        pltpu.make_async_copy(
            cov.at[pl.ds(start, stop - start), :],
            ext.at[pl.ds(16 + start, stop - start), own],
            load_sem,
        ).start()
    fog_loads = [
        pltpu.make_async_copy(fogr, fr, fog_sem.at[0]),
        pltpu.make_async_copy(fogc, fc, fog_sem.at[1]),
    ]
    for copy in fog_loads:
        copy.start()

    def whole(ref, sem):
        pltpu.make_async_copy(ref, ref, sem).wait()

    ext[0:16, :] = jnp.zeros((16, cols + 256), I32)
    ext[272:288, :] = jnp.zeros((16, cols + 256), I32)
    ext[16:272, 0:128] = jnp.zeros((256, 128), I32)
    ext[16:272, cols + 128 : cols + 256] = jnp.zeros((256, 128), I32)
    for buf in (mext, bext):
        buf[0:48, :] = jnp.zeros((48, 128), F32)
        buf[112:160, :] = jnp.zeros((48, 128), F32)

    def at(x, y, c):
        return (stripe, x * SIDE + y, c)

    def beside_y(d):
        return lax.rem(py + d, SIDE)

    def beside_x(d):
        return lax.rem(px + d, SIDE)

    barrier = pltpu.get_barrier_semaphore()

    def signal(sem, target):
        pl.semaphore_signal(sem, inc=1, device_id=target, device_id_type=MESH)

    crosses_up = jnp.logical_and(py == 0, px > 0)
    crosses_down = jnp.logical_and(py == SIDE - 1, px < SIDE - 1)
    for d in (7, 1):
        for c in (0, 1):
            signal(barrier, at(px, beside_y(d), c))
        signal(barrier, at(beside_x(d), py, col))
    signal(barrier, at(px, py, other))

    @pl.when(crosses_up)
    def _():
        for c in (0, 1):
            signal(barrier, (stripe, row - 1, c))

    @pl.when(crosses_down)
    def _():
        for c in (0, 1):
            signal(barrier, (stripe, row + 1, c))

    def send(src, dst, s_sem, r_sem, target):
        pltpu.make_async_remote_copy(
            src_ref=src, dst_ref=dst, send_sem=s_sem, recv_sem=r_sem,
            device_id=target, device_id_type=MESH,
        ).start()

    inner = pl.ds(pl.multiple_of((1 - col) * (cols - 128) + 128, 128), 128)
    pad_there = pl.ds(pl.multiple_of(col * (cols + 128), 128), 128)
    pad_here = pl.ds(pl.multiple_of(other * (cols + 128), 128), 128)
    body, top, bottom = pl.ds(16, 256), pl.ds(8, 8), pl.ds(272, 8)
    both = pl.ds(0, cols + 128)
    up, down = row > 0, row < last

    for i in range(cols // 256):
        part = (iota((256, 128), 0) + 256 * i) // BS
        s1[256 * i : 256 * i + 256, :] = onehot(part == iota((256, 128), 1)).astype(BF16)
    wh, wl = split(taps_of(iota((256, 128), 0) - iota((256, 128), 1) - 64))
    wcat[:, 0:128] = wh
    wcat[:, 128:256] = wl
    bh, bl = split(taps_of(iota((144, 160), 1) - iota((144, 160), 0) - 16))
    b16[0:144, :] = bh
    b16[144:288, :] = bl
    for i in range(wide // 128):
        part = (iota((128, 128), 0) + 128 * i - 64) // BS
        inside = jnp.logical_and(part >= 0, part < cells)
        s2[128 * i : 128 * i + 128, :] = onehot(
            jnp.logical_and(inside, part == iota((128, 128), 1))
        ).astype(BF16)

    whole(ext.at[pl.ds(16, 16), own], edge_sem)
    pl.semaphore_wait(
        barrier,
        7 + 2 * crosses_up.astype(I32) + 2 * crosses_down.astype(I32),
    )

    for d in (1, 7):
        signal(ready.at[0], at(px, beside_y(d), col))
        signal(ready.at[0], at(beside_x(d), py, col))

    @pl.when(up)
    def _():
        send(ext.at[first8, own], ext.at[bottom, own], halo_send.at[1], halo_recv.at[1], (stripe, row - 1, col))
        send(ext.at[first8, inner], ext.at[bottom, pad_there], halo_send.at[1], halo_recv.at[1], (stripe, row - 1, other))

    @pl.when(down)
    def _():
        send(ext.at[last8, own], ext.at[top, own], halo_send.at[2], halo_recv.at[2], (stripe, row + 1, col))
        send(ext.at[last8, inner], ext.at[top, pad_there], halo_send.at[2], halo_recv.at[2], (stripe, row + 1, other))

    for i in range(8):
        if i == 0:
            whole(ext.at[pl.ds(24, 240), own], load_sem)
        x = ext[16 + 32 * i : 48 + 32 * i, 128 : cols + 128].astype(F32)
        rs[8 * i : 8 * i + 8, :] = x.reshape(4, 8, cols).sum(axis=0)
        cb[16 + 32 * i : 48 + 32 * i, 128 : cols + 128] = x.astype(BF16)
    sums = dot_exact(rs[...], s1[...])
    means = sums.reshape(8, 8, 128).sum(axis=1) * (1.0 / (255.0 * BS * BS))
    mbuf[mine] = packed(means)

    send(ext.at[body, inner], ext.at[body, pad_there], halo_send.at[0], halo_recv.at[0], at(px, py, other))

    def spread_y(buf, sem, order, partner):
        for d in order:
            for c in (0, 1):
                send(buf.at[mine], buf.at[mine], sem.at[0], sem.at[1], at(px, beside_y(d), c))
        if partner:
            send(buf.at[mine], buf.at[mine], sem.at[0], sem.at[1], at(px, py, other))

    def collect_y(buf, sem):
        whole(buf.at[pl.ds(0, 2 * SIDE - 1)], sem.at[1])

    def spread_x(buf, sem):
        for d in ORDER:
            send(buf.at[px], buf.at[px], sem.at[0], sem.at[1], at(beside_x(d), py, col))

    def collect_x(buf, sem):
        whole(buf.at[pl.ds(0, SIDE - 1)], sem.at[1])

    def spread_slabs(buf, sem):
        @pl.when(px < SIDE - 1)
        def _():
            send(buf.at[pl.ds(64, 48), :], buf.at[pl.ds(0, 48), :],
                 sem.at[0], sem.at[2], at(px + 1, py, col))

        @pl.when(px > 0)
        def _():
            send(buf.at[pl.ds(48, 48), :], buf.at[pl.ds(112, 48), :],
                 sem.at[1], sem.at[3], at(px - 1, py, col))

    def collect_slabs(buf, sem):
        @pl.when(px > 0)
        def _():
            whole(buf.at[pl.ds(0, 48), :], sem.at[2])

        @pl.when(px < SIDE - 1)
        def _():
            whole(buf.at[pl.ds(112, 48), :], sem.at[3])

    def pieces(ref, parts, lanes):
        found = [ref[first : first + count, lanes] for first, count in parts]
        return found[0] if len(found) == 1 else jnp.concatenate(found, axis=0)

    def put(ref, parts, lanes, value):
        at_row = 0
        for first, count in parts:
            ref[first : first + count, lanes] = value[at_row : at_row + count]
            at_row += count

    def blur_across(src_hi, src_lo, dst_hi, dst_lo, parts, tiles):
        for j in range(tiles):
            window, lanes = slice(128 * j, 128 * j + 256), slice(128 * j, 128 * j + 128)
            wide_part = dot(pieces(src_hi, parts, window), wcat[...])
            part = wide_part[:, 0:128] + wide_part[:, 128:256]
            if src_lo is not None:
                part = part + dot(pieces(src_lo, parts, window), wcat[:, 0:128])
            high, low = split(part)
            put(dst_hi, parts, lanes, high)
            put(dst_lo, parts, lanes, low)

    def shift_coverage(parts):
        count = sum(n for _, n in parts)
        half = iota((count, 128), 1) < 64
        turned = pltpu.roll(pieces(ext, parts, slice(0, 128)).astype(F32), 64, 1)
        for j in range(wide // 128):
            following = pieces(ext, parts, slice(128 * j + 128, 128 * j + 256)).astype(F32)
            following = pltpu.roll(following, 64, 1)
            put(cs, parts, slice(128 * j, 128 * j + 128), jnp.where(half, turned, following))
            turned = following

    def blur_down(count, depth, high, low, first, lanes):
        both = jnp.concatenate([b16[0:count, 0:depth], b16[144 : 144 + count, 0:depth]], 0)
        here = slice(first, first + depth)
        result = dot(both, high[here, lanes])
        return result[0:count] + result[count:] + dot(b16[0:count, 0:depth], low[here, lanes])

    pl.semaphore_wait(ready.at[0], 4)
    for d in (2, 6):
        signal(ready.at[1], at(px, beside_y(d), col))
        signal(ready.at[1], at(beside_x(d), py, col))

    spread_y(mbuf, m_sem, (2, 6, 1, 7), True)
    body_rows, edge_rows = ((16, 256),), ((0, 16), (272, 16))
    whole(ext.at[body, pad_here], halo_recv.at[0])
    for pad in (0, cols + 128):
        cb[16:272, pad : pad + 128] = ext[16:272, pad : pad + 128].astype(F32).astype(BF16)
    blur_across(cb, None, hhi, hlo, body_rows, wide // 128)

    shift_coverage(body_rows)

    tiles = [slice(256 * j, 256 * j + 256) for j in range(wide // 256)]
    if wide % 256:
        tiles.append(slice(wide - 128, wide))

    def main_rows(lanes):
        width = lanes.stop - lanes.start
        for block in (0, 1):
            here = slice(32 + 112 * block, 144 + 112 * block)
            t = 1.5 - blur_down(112, 144, hhi, hlo, 16 + 112 * block, lanes) * (0.5 / 255.0)
            tt[here, lanes] = t
            product = cs[here, lanes] * t
            whole = product[16:112] if block == 0 else product[0:96]
            half = product[0:16] if block == 0 else product[96:112]
            whole = whole.reshape(3, 4, 8, width).sum(axis=1).reshape(24, width)
            asum[8 + 24 * block : 32 + 24 * block, lanes] = whole
            asum[56 * block : 56 * block + 8, lanes] = half[0:8] + half[8:16]

    for lanes in tiles:
        main_rows(lanes)

    pl.semaphore_wait(ready.at[1], 4)
    spread_y(mbuf, m_sem, (4, 3, 5), False)

    part, side = iota((128, 192), 0) // 64, lax.rem(iota((128, 192), 0) // 32, 2)
    piece = iota((128, 192), 1) // 48
    value = taps_of(lax.rem(iota((128, 192), 1), 48) - lax.rem(iota((128, 192), 0), 32) - 16 * side)
    high, low = split(value)
    value = jnp.where(part == 0, high.astype(F32), jnp.where(lax.rem(piece, 2) == 0, low.astype(F32), 0.0))
    edge_taps = jnp.where(side == piece // 2, value, 0.0).astype(BF16)


    @pl.when(up)
    def _():
        whole(ext.at[top, both], halo_recv.at[2])

    @pl.when(down)
    def _():
        whole(ext.at[bottom, both], halo_recv.at[1])

    for first in (0, 272):
        cb[first : first + 16, :] = ext[first : first + 16, :].astype(F32).astype(BF16)
    blur_across(cb, None, hhi, hlo, edge_rows, wide // 128)
    shift_coverage(edge_rows)
    for lanes in tiles:
        inputs = jnp.concatenate(
            [hhi[0:48, lanes], hlo[0:48, lanes], hhi[240:288, lanes], hlo[240:288, lanes]], 0
        )
        result = dot(edge_taps, inputs)
        t = 1.5 - (result[0:64] + result[64:128]) * (0.5 / 255.0)
        tt[0:32, lanes] = t[0:32]
        tt[256:288, lanes] = t[32:64]
        product = cs[16:32, lanes] * t[16:32]
        asum[64:72, lanes] = product[0:8] + product[8:16]
        product = cs[256:272, lanes] * t[32:48]
        asum[72:80, lanes] = product[0:8] + product[8:16]
    sums = dot_exact(asum[...], s2[...]).reshape(10, 8, 128).sum(axis=1)
    cell_row = iota((8, 128), 0)
    sums = (
        sums[0:8]
        + jnp.where(cell_row == 0, sums[8:9], 0.0)
        + jnp.where(cell_row == 7, sums[9:10], 0.0)
    )
    abuf[mine] = packed(sums * (1.0 / (255.0 * BS * BS)))
    spread_y(abuf, a_sem, ORDER, True)

    collect_y(mbuf, m_sem)
    mx = unpacked(mbuf)
    mext[48:112, :] = mx
    to_region = jnp.where(
        iota((128, 128), 0) // 8 == lax.rem(iota((128, 128), 1), 16), 1.0 / 64.0, 0.0
    ).astype(BF16)
    own_lanes = iota((64, 128), 1) // 16 == iota((64, 128), 0) // 8

    def region_row(field):
        return jnp.where(own_lanes, dot_exact(field, to_region), 0.0).sum(axis=0, keepdims=True)

    pbuf[px] = region_row(mx)
    spread_slabs(mext, ms_sem)
    spread_x(pbuf, p_sem)
    for i in range(wide // 128):
        cell = (iota((128, 128), 1) + 128 * i + cols * col - 64 + 128) // BS - 4
        sps[:, 128 * i : 128 * i + 128] = onehot(cell == iota((128, 128), 0)).astype(BF16)

    across = gauss_of(iota((128, 128), 0) - iota((128, 128), 1))
    across = jnp.where(
        jnp.logical_and(iota((128, 128), 0) < 2 * cells, iota((128, 128), 1) < 2 * cells), across, 0.0
    )
    ah, al = split(across)

    def dot_across(field):
        fh, fl = split(field)
        return dot(fh, ah) + (dot(fl, ah) + dot(fh, al))

    for copy in fog_loads:
        copy.wait()
    kr = fr[...]
    kr = kr / jnp.sum(kr, axis=1, keepdims=True)
    kc = fc[...]
    kc = kc / jnp.sum(kc, axis=1, keepdims=True)
    nreg = 2 * cells // 8
    pick = onehot(lax.rem(iota((128, nreg), 0), 16) == iota((128, nreg), 1))
    kct = kc.T
    to_cells = dot_exact(kct, onehot(iota((nreg, 128), 1) // 8 == iota((nreg, 128), 0)))
    to_lanes = dot_exact(kct, onehot(lax.rem(iota((nreg, 128), 1), 16) == iota((nreg, 128), 0)))
    zc = exact_dot(pick, to_cells)
    zl = exact_dot(pick, to_lanes)
    zboth = jnp.concatenate([zc, zl], axis=1)
    in_block = iota((64, 128), 1) // 16 == lax.rem(iota((64, 128), 0), 8)
    kr_24 = exact_dot(onehot(row - 1 + iota((24, 64), 0) // 8 == iota((24, 64), 1)), kr)
    kr_160 = exact_dot(onehot(8 * px - 6 + iota((160, 64), 0) // 8 == iota((160, 64), 1)), kr)
    own_kr = jnp.where(iota((64, 64), 0) == row, kr, 0.0).sum(axis=0, keepdims=True)
    own_kr = jnp.where(iota((8, 64), 1) // 8 == iota((8, 64), 0), own_kr, 0.0)
    own_kr = dot_exact(own_kr, onehot(lax.rem(iota((64, 128), 0), 8) == iota((64, 128), 1) // 16))
    zph, zpl = split(dot_exact(0.2 * zc, sps[:, 64 : cols + 64]))
    zp[0] = zph
    zp[1] = zpl

    collect_slabs(mext, ms_sem)
    swept = dot_across(mext[...])
    back_x = dot3(gauss_of(iota((64, 160), 0) - iota((64, 160), 1) + 48), swept)
    back_24 = dot3(gauss_of(iota((24, 160), 0) - iota((24, 160), 1) + 40 + 8 * py), swept)

    collect_y(abuf, a_sem)
    ax = unpacked(abuf)
    bx = ax - 0.3 * back_x * mext[48:112, :]
    bext[48:112, :] = bx
    ebuf[px] = region_row(bx)
    spread_x(ebuf, e_sem)
    spread_slabs(bext, bs_sem)

    collect_x(pbuf, p_sem)
    regions = pbuf[...]
    spread = jnp.broadcast_to(regions, (8, 8, 128)).reshape(64, 128)
    fog_wide = dot3(jnp.where(in_block, spread, 0.0), zboth)
    fog_24 = dot3(kr_24, fog_wide[:, 0:128])

    coarse = 0.3 * back_24 + 0.2 * fog_24
    row24[...] = dot_exact(coarse, sps[...])
    fog_lanes = jnp.where(in_block, dot3(kr, fog_wide[:, 128:256]), 0.0).reshape(8, 8, 128).sum(axis=1)
    fog_160 = dot3(kr_160, fog_wide[:, 0:128])
    for first, count, place in [(0, 16, 7)] + [(16 + 32 * i, 32, 8 + i) for i in range(8)] + [(272, 16, 16)]:
        here = slice(first, first + count)
        high, low = split(cs[here, :] * (tt[here, :] - row24[place : place + 1, :]))
        qhi[here, :] = high
        qlo[here, :] = low
    blur_across(qhi, qlo, h2hi, h2lo, ((0, 288),), cols // 128)
    left = iota((128, 128), 1) < 64
    for j in range(cols // 256):
        lanes = slice(256 * j, 256 * j + 256)
        for block in (0, 1):
            fine = blur_down(128, 160, h2hi, h2lo, 128 * block, lanes)
            here = slice(16 + 128 * block, 144 + 128 * block)
            turned = [pltpu.roll(tt[here, 256 * j + 128 * i : 256 * j + 128 * i + 128], 64, 1) for i in range(3)]
            for i in (0, 1):
                dose = jnp.where(left, turned[i], turned[i + 1])
                x_out[128 * block : 128 * block + 128, 256 * j + 128 * i : 256 * j + 128 * i + 128] = (
                    dose + 0.5 - fine[:, 128 * i : 128 * i + 128] * (0.5 / 255.0)
                )

    whole(mbuf.at[pl.ds(0, 2 * SIDE - 1)], m_sem.at[0])
    whole(abuf.at[pl.ds(0, 2 * SIDE - 1)], a_sem.at[0])
    whole(pbuf.at[pl.ds(0, SIDE - 1)], p_sem.at[0])
    whole(ebuf.at[pl.ds(0, SIDE - 1)], e_sem.at[0])
    whole(ext.at[body, pad_here], halo_send.at[0])

    @pl.when(up)
    def _():
        whole(ext.at[top, both], halo_send.at[1])

    @pl.when(down)
    def _():
        whole(ext.at[bottom, both], halo_send.at[2])

    @pl.when(px < SIDE - 1)
    def _():
        whole(mext.at[pl.ds(0, 48), :], ms_sem.at[0])
        whole(bext.at[pl.ds(0, 48), :], bs_sem.at[0])

    @pl.when(px > 0)
    def _():
        whole(mext.at[pl.ds(112, 48), :], ms_sem.at[1])
        whole(bext.at[pl.ds(112, 48), :], bs_sem.at[1])

    collect_slabs(bext, bs_sem)
    means2 = bext[...] - 0.2 * fog_160 * mext[...]
    back2 = dot3(gauss_of(iota((8, 160), 0) - iota((8, 160), 1) + 48 + 8 * py), dot_across(means2))
    coarse_out[...] = dot_exact(0.3 * back2 + coarse[8:16], sps[:, 64 : cols + 64])
    fog_known = 0.2 * fog_lanes * regions.reshape(8, 128)
    collect_x(ebuf, e_sem)
    fog_mean2 = ebuf[...].reshape(8, 128) - fog_known
    weighted = jnp.broadcast_to((own_kr * fog_mean2).sum(axis=0, keepdims=True), (8, 128))
    high, low = split(weighted)
    fog2 = dot(high, zp[0]) + (dot(low, zp[0]) + dot(high, zp[1]))
    coarse_out[...] = coarse_out[...] + fog2


def finish_kernel(x, coarse, out, buf, sem):
    cols = coarse.shape[1]
    copies = []
    for i in range(8):
        here = pl.ds(32 * i, 32)
        buf[32 * i : 32 * i + 32, :] = x[32 * i : 32 * i + 32, :] - coarse[i : i + 1, :]
        copy = pltpu.make_async_copy(buf.at[here, :], out.at[here, :], sem.at[i])
        copy.start()
        copies.append(copy)
    for copy in copies:
        copy.wait()


def shards(coverage, fog_rows, fog_cols):
    rows, cols = coverage.shape
    wide = cols + 128
    dma = pltpu.SemaphoreType.DMA
    hbm = pl.BlockSpec(memory_space=pl.ANY)
    vmem = pl.BlockSpec(memory_space=pltpu.VMEM)
    x, coarse = pl.pallas_call(
        correct_kernel,
        out_shape=(
            jax.ShapeDtypeStruct((rows, cols), F32),
            jax.ShapeDtypeStruct((8, cols), F32),
        ),
        in_specs=[pl.BlockSpec(memory_space=pltpu.MemorySpace.HBM)] * 3,
        out_specs=(vmem, vmem),
        scratch_shapes=[
            pltpu.VMEM((288, cols + 256), I32),
            pltpu.VMEM((288, cols + 256), BF16),
            pltpu.VMEM((64, cols), F32),
            pltpu.VMEM((288, wide), F32),
            pltpu.VMEM((288, wide), BF16),
            pltpu.VMEM((288, wide), BF16),
            pltpu.VMEM((288, wide), F32),
            pltpu.VMEM((80, wide), F32),
            pltpu.VMEM((288, wide), BF16),
            pltpu.VMEM((288, wide), BF16),
            pltpu.VMEM((288, cols), BF16),
            pltpu.VMEM((288, cols), BF16),
            pltpu.VMEM((cols, 128), BF16),
            pltpu.VMEM((wide, 128), BF16),
            pltpu.VMEM((128, wide), BF16),
            pltpu.VMEM((256, 256), BF16),
            pltpu.VMEM((288, 160), BF16),
            pltpu.VMEM((2, 128, cols), BF16),
            pltpu.VMEM((24, wide), F32),
            pltpu.VMEM((2 * SIDE, 4, 128), F32),
            pltpu.VMEM((160, 128), F32),
            pltpu.VMEM((SIDE, 1, 128), F32),
            pltpu.VMEM((2 * SIDE, 4, 128), F32),
            pltpu.VMEM((160, 128), F32),
            pltpu.VMEM((SIDE, 1, 128), F32),
            pltpu.VMEM(fog_rows.shape, F32),
            pltpu.VMEM(fog_cols.shape, F32),
            dma(()), dma(()), dma((2,)), dma((3,)), dma((3,)), pltpu.SemaphoreType.REGULAR((2,)),
            dma((2,)), dma((2,)), dma((2,)), dma((2,)), dma((4,)), dma((4,)),
        ],
        compiler_params=pltpu.CompilerParams(
            collective_id=0, has_side_effects=True, vmem_limit_bytes=44 * 1024 * 1024
        ),
    )(*[pltpu.with_memory_space_constraint(v, pltpu.MemorySpace.HBM) for v in (coverage, fog_rows, fog_cols)])
    return pl.pallas_call(
        finish_kernel,
        out_shape=jax.ShapeDtypeStruct((rows, cols), F32),
        in_specs=[vmem, vmem],
        out_specs=hbm,
        scratch_shapes=[pltpu.VMEM((rows, cols), F32), dma((8,))],
        compiler_params=pltpu.CompilerParams(vmem_limit_bytes=8 * 1024 * 1024),
    )(x, coarse)


def solution(mesh):
    placed = (P(("stripe", "row"), "col"), P(), P())
    return jax.shard_map(
        shards, mesh=mesh, in_specs=placed, out_specs=P(("stripe", "row"), "col"), check_vma=False
    )
```
